32 devices in a mesh: gx: 4 (over z), gy: 4 (over y, x), gz: 2 (over core).
Axes of the slice: x: 2, y: 2, z: 4, core: 2. Of those that a mesh axis runs over, the one named last changes fastest.
Arguments:
- east_wind: float32 [96, 512, 512], P('gz', 'gx', 'gy'), may hold values from -6 to 6
- north_wind: float32 [96, 512, 512], P('gz', 'gx', 'gy'), may hold values from -6 to 6
- vertical_wind: float32 [96, 512, 512], P('gz', 'gx', 'gy'), may hold values from -6 to 6
- geopotential: float32 [96, 512, 512], P('gz', 'gx', 'gy'), may hold values from -6 to 6
- pressure: float32 [96, 512, 512], P('gz', 'gx', 'gy'), may hold values from -6 to 6
- column_mass: float32 [512, 512], P('gx', 'gy'), may hold values from 0.5 to 2
Outputs:
- east_after: float32 [96, 512, 512], P('gz', 'gx', 'gy')
- north_after: float32 [96, 512, 512], P('gz', 'gx', 'gy')
- vertical_after: float32 [96, 512, 512], P('gz', 'gx', 'gy')
- geo_after: float32 [96, 512, 512], P('gz', 'gx', 'gy')
- pressure_after: float32 [96, 512, 512], P('gz', 'gx', 'gy')
The draws below stay inside these ranges and needn't reach their ends.
All inputs are finite; a program needn't handle non-finite values.
Results may differ from the reference program's by a relative error of at most 0.0003.
Values sent between devices are 32-bit elements; how exact they have to be, the bound alone decides.
A program may use at most 128 MiB of HBM per device.

```python
import math
import jax
import jax.numpy as jnp
from jax import lax

NZ = 96
ITERS = 3
NX = 512
NY = 512


def draw_vertical_wind(key, part):
    key_noise = jax.random.fold_in(key, 11)
    noise = jax.random.truncated_normal(key_noise, -6.0, 6.0, (NZ, NX, NY), jnp.float32)
    return noise


def steps_of(own_key, dims, shards, low, top_value):
    gain, own = 1.0, jax.random.fold_in(own_key, 6)
    for dim, blocks in shards:
        draws = jnp.exp(jax.random.uniform(jax.random.fold_in(own, dim), (blocks,), jnp.float32, low / len(shards), top_value / len(shards)))
        gain = gain * jnp.repeat(draws, dims[dim] // blocks).reshape([-1 if axis == dim else 1 for axis in range(len(dims))])
    return gain


def bell_draw(rng, shape, spread, reach, pieces=(), held_as=jnp.bfloat16):
    gain = steps_of(rng, shape, pieces, -0.22, 0.18) if pieces else 1.0
    drawn = jax.random.normal(rng, shape, jnp.float32) * spread * gain
    return jnp.minimum(jnp.maximum(drawn, -reach), reach).astype(held_as)


def setup_inputs(seed: int = 0) -> dict:
    seeds = jax.random.split(jax.random.key(seed), 7)
    return {
        "east_wind": bell_draw(seeds[0], (NZ, NX, NY), 1.0, 6.0, ((0, 2), (1, 4), (2, 4)), jnp.float32),
        "north_wind": bell_draw(seeds[1], (NZ, NX, NY), 1.0, 6.0, ((0, 2), (1, 4), (2, 4)), jnp.float32),
        "vertical_wind": draw_vertical_wind(jax.random.fold_in(seeds[6], 71), 0),
        "geopotential": bell_draw(seeds[3], (NZ, NX, NY), 1.0, 6.0, ((0, 2), (1, 4), (2, 4)), jnp.float32),
        "pressure": bell_draw(seeds[4], (NZ, NX, NY), 1.0, 6.0, ((0, 2), (1, 4), (2, 4)), jnp.float32),
        "column_mass": jnp.clip(jnp.exp(math.log(2.0) - 1.3862944 * jax.random.uniform(seeds[5], (NX, NY), jnp.float32) ** steps_of(seeds[5], (NX, NY), ((0, 4), (1, 4)), -0.2, 0.2)), 0.5, 2.0),
    }


horiz_push = 0.25
mass_flux = 0.2
level_push = 1.0
buoy_coupling = 0.5
geo_rate = 0.5
level_flux = 0.5
stiffness = 30.0


def centered(source, dim_index):
    return jnp.roll(source, -1, dim_index) - jnp.roll(source, 1, dim_index)


def level_diff(source):
    zeros_level = jnp.zeros_like(source[:1])
    shifted_up = jnp.concatenate([source[1:], zeros_level], 0)
    shifted_down = jnp.concatenate([zeros_level, source[:-1]], 0)
    return shifted_up - shifted_down


def column_solve(forcing, stiff_ratio):
    diagonal = 1.0 + 2.0 * stiff_ratio

    def forward(carried, forcing_row):
        coef_prev, rhs_prev = carried
        pivot_row = diagonal + stiff_ratio * coef_prev
        coef_next = -stiff_ratio / pivot_row
        rhs_next = (forcing_row + stiff_ratio * rhs_prev) / pivot_row
        return (coef_next, rhs_next), (coef_next, rhs_next)

    zeros_plane = jnp.zeros_like(stiff_ratio)
    _, (coefs, rhs_rows) = lax.scan(forward, (zeros_plane, zeros_plane), forcing)

    def backward(next_value, level_item):
        coef_row, rhs_row = level_item
        solved = rhs_row - coef_row * next_value
        return solved, solved

    _, solved = lax.scan(backward, zeros_plane, (coefs, rhs_rows), reverse=True)
    return solved


def reference(east_wind, north_wind, vertical_wind, geopotential, pressure, column_mass):
    stiff_ratio = stiffness * column_mass
    for substep in range(ITERS):
        east_wind = east_wind - horiz_push * centered(pressure, 1)
        north_wind = north_wind - horiz_push * centered(pressure, 2)
        divergence = centered(east_wind, 1) + centered(north_wind, 2)
        pressure_star = pressure - mass_flux * column_mass * divergence
        forcing = vertical_wind - level_push * level_diff(pressure_star) + buoy_coupling * geopotential
        vertical_wind = column_solve(forcing, stiff_ratio)
        geopotential = geopotential + geo_rate * vertical_wind
        pressure = pressure_star - level_flux * column_mass * level_diff(vertical_wind)
    return east_wind, north_wind, vertical_wind, geopotential, pressure
```

```python
import functools

import jax
import jax.numpy as jnp
from jax import lax
from jax.experimental import pallas as pl
from jax.experimental.pallas import tpu as pltpu
from jax.sharding import PartitionSpec as P

ITERS = 3
STIFF = 30.0
PAD = 8
ROWS = 16
PARTS = 2
UNROLL = 24


def roll(value, shift):
    if isinstance(shift, int):
        shift = shift % value.shape[1]
    return pltpu.roll(value, shift, 1)


def kernel(n, ni, nj, sizes, east_in, north_in, vert_in, geo_in, press_in, mass,
           east, north, vert, geo, press,
           pp, up, psum, dvg, mu_s, c_s, planes, bounds,
           row_out, row_in, col_out, col_in, z_out, z_in,
           load_sem, row_send, row_recv, col_send, col_recv, z_send, z_recv):
    nx, ny, nz = sizes
    unroll = max(u for u in range(2, UNROLL + 1) if n % u == 0 and u % 2 == 0)
    ix, iy, iz = lax.axis_index("gx"), lax.axis_index("gy"), lax.axis_index("gz")
    xs = (lax.rem(ix + nx - 1, nx), lax.rem(ix + 1, nx))
    ys = (lax.rem(iy + ny - 1, ny), lax.rem(iy + 1, ny))

    loads = [
        pltpu.make_async_copy(press_in, pp.at[:, pl.ds(PAD, ni), :], load_sem.at[0]),
        pltpu.make_async_copy(east_in, up.at[:, pl.ds(PAD, ni), :], load_sem.at[1]),
        pltpu.make_async_copy(north_in, north, load_sem.at[2]),
        pltpu.make_async_copy(vert_in, vert, load_sem.at[3]),
        pltpu.make_async_copy(geo_in, geo, load_sem.at[4]),
    ]
    for load in loads:
        load.start()

    barrier = pltpu.get_barrier_semaphore()
    for t in range(2):
        pl.semaphore_signal(barrier, inc=1, device_id={"gx": xs[t]})
        pl.semaphore_signal(barrier, inc=1, device_id={"gy": ys[t]})
    for d in range(1, nz):
        pl.semaphore_signal(barrier, inc=1, device_id={"gz": lax.rem(iz + d, nz)})
    pl.semaphore_wait(barrier, 4 + nz - 1)

    def row_copy(slot, t):
        return pltpu.make_async_remote_copy(
            src_ref=row_out.at[slot, t], dst_ref=row_in.at[slot, 1 - t],
            send_sem=row_send.at[slot, t], recv_sem=row_recv.at[slot, 1 - t],
            device_id={"gx": xs[t]})

    span = ni // PARTS

    def part_rows(h):
        return pl.ds(pl.multiple_of(h * span, span), span)

    def col_copy(slot, t, h):
        return pltpu.make_async_remote_copy(
            src_ref=col_out.at[slot, t, part_rows(h), :], dst_ref=col_in.at[slot, 1 - t, part_rows(h), :],
            send_sem=col_send.at[slot, t, h], recv_sem=col_recv.at[slot, 1 - t, h],
            device_id={"gy": ys[t]})

    def z_copy(slot, d, h):
        return pltpu.make_async_remote_copy(
            src_ref=z_out.at[slot, :, part_rows(h), :], dst_ref=z_in.at[slot, d - 1, :, part_rows(h), :],
            send_sem=z_send.at[slot, d - 1, h], recv_sem=z_recv.at[slot, d - 1, h],
            device_id={"gz": lax.rem(iz + d, nz)})

    lane = lax.broadcasted_iota(jnp.int32, (ROWS, nj), 1)
    pair = lane // 2

    def merged(left, right, width):
        left, right = roll(left, width), roll(right, nj - width)
        even = pair % 2 == 0
        return jnp.where(even, right, left), jnp.where(even, left, right)

    def send_rows(slot, ref):
        row_out[slot, 0] = ref[:, PAD : PAD + 2, :]
        row_out[slot, 1] = ref[:, PAD + ni - 2 : PAD + ni, :]
        for t in range(2):
            row_copy(slot, t).start()

    def recv_rows(slot, ref):
        for t in range(2):
            row_copy(slot, t).wait()
        ref[:, PAD - 2 : PAD, :] = row_in[slot, 0]
        ref[:, PAD + ni : PAD + ni + 2, :] = row_in[slot, 1]

    def packed(value, k, packs):
        turned = roll(value, 2 * k + 2)
        return (jnp.where(pair == k + 1, turned, packs[0]), jnp.where(pair == k, turned, packs[1]))

    def strips(body, h=None):
        count = (ni if h is None else span) // ROWS
        first = 0 if h is None else h * count

        @pl.loop(0, count)
        def _(s):
            body(pl.multiple_of((first + s) * ROWS, ROWS))

    def send_cols(slot, load_level):
        def body(r0):
            zero = jnp.zeros((ROWS, nj), jnp.float32)

            def group(q, packs):
                for e in range(unroll):
                    k = q * unroll + e
                    packs = packed(load_level(k, r0), k, packs)
                return packs

            packs = lax.fori_loop(0, n // unroll, group, (zero, zero))
            for t in range(2):
                col_out[slot, t, pl.ds(r0, ROWS), :] = packs[t]

        strips(body)
        for h in range(PARTS):
            for t in range(2):
                col_copy(slot, t, h).start()

    loads[0].wait()
    send_rows(0, pp)
    send_cols(0, lambda k, r0: pp[k, pl.ds(PAD + r0, ROWS), :])
    loads[1].wait()
    send_rows(ITERS, up)
    loads[2].wait()
    send_cols(ITERS, lambda k, r0: north[k, pl.ds(r0, ROWS), :])

    stiff = STIFF * mass[...]
    root = jnp.sqrt(1.0 + 4.0 * stiff)
    major = 0.5 * (1.0 + 2.0 * stiff + root)
    mu_s[...] = stiff / major
    c_s[...] = 1.0 / major
    planes[0] = jnp.log(stiff / major)
    planes[1] = major / root
    planes[2] = major / stiff

    recv_rows(0, pp)
    recv_rows(ITERS, up)
    for slot in (0, ITERS):
        for t in range(2):
            for h in range(PARTS):
                col_copy(slot, t, h).wait()
    loads[3].wait()
    loads[4].wait()

    def pass_one(it, h):
        def body(r0):
            rows = pl.ds(r0, ROWS)
            m, mu, c = mass[rows, :], mu_s[rows, :], c_s[rows, :]
            weak, strong = 0.05 * m, 0.2 * m
            left, right = col_in[it, 0, rows, :], col_in[it, 1, rows, :]
            ends = merged(left, right, 2)
            if it == 0:
                vends = merged(col_in[ITERS, 0, rows, :], col_in[ITERS, 1, rows, :], 1)

            def star(k, parity):
                end = roll(ends[parity], nj - 2 - 2 * k)
                at = pl.ds(PAD + r0, ROWS)
                p = pp[k, at, :]
                low = jnp.where(lane < 2, end, roll(p, 2))
                high = jnp.where(lane >= nj - 2, end, roll(p, nj - 2))
                total = (pp[k, pl.ds(PAD + r0 + 2, ROWS), :] + pp[k, pl.ds(PAD + r0 - 2, ROWS), :]) + (low + high) - 4.0 * p
                if it == 0:
                    v = north[k, rows, :]
                    vend = roll(vends[parity], nj - 2 - 2 * k)
                    vlow = jnp.where(lane < 1, vend, roll(v, 1))
                    vhigh = jnp.where(lane >= nj - 1, vend, roll(v, nj - 1))
                    d = strong * (up[k, pl.ds(PAD + r0 + 1, ROWS), :] - up[k, pl.ds(PAD + r0 - 1, ROWS), :] + (vhigh - vlow))
                    psum[k, at, :] = p
                else:
                    d = dvg[k, rows, :]
                    psum[k, at, :] = psum[k, at, :] + p
                d = d - weak * total
                if it < ITERS - 1:
                    dvg[k, rows, :] = d
                ps = p - d
                press[k, rows, :] = ps
                return ps

            def sweep(k, above, below, state):
                y, dn, weight = state
                f = c * (vert[k, rows, :] + 0.5 * geo[k, rows, :] - (above - below))
                y = mu * y + f
                vert[k, rows, :] = y
                return y, dn + weight * f, weight * mu

            def steps(ks, carry):
                older, newer, state = carry
                for e, k in enumerate(ks):
                    ps = star(k, e % 2)
                    if not (isinstance(k, int) and k == 0):
                        state = sweep(k - 1, ps, older, state)
                    older, newer = newer, ps
                return older, newer, state

            zero = jnp.zeros((ROWS, nj), jnp.float32)
            carry = (zero, zero, (zero, zero, zero + 1.0))
            carry = steps(range(unroll), carry)
            planes_lo = press[0, rows, :]

            def group(q, carry):
                return steps([q * unroll + e for e in range(unroll)], carry)

            older, newer, state = lax.fori_loop(1, n // unroll, group, carry)
            y, dn, _ = sweep(n - 1, zero, older, state)
            z_out[it, 0, rows, :] = y
            z_out[it, 1, rows, :] = dn
            z_out[it, 2, rows, :] = c * planes_lo
            z_out[it, 3, rows, :] = c * newer

        strips(body, h)

    def interface(it, h):
        def body(r0):
            rows = pl.ds(r0, ROWS)
            mu, logmu, kappa, inv = mu_s[rows, :], planes[0, rows, :], planes[1, rows, :], planes[2, rows, :]
            zero = jnp.zeros((ROWS, nj), jnp.float32)

            def power(m):
                if not isinstance(m, int):
                    m = jnp.maximum(m, 0).astype(jnp.float32)
                return jnp.exp(m * logmu)

            near = power(n - 1)
            below, above, to_low, to_high = zero, zero, zero, zero
            pieces = {}

            def piece(d, which):
                if abs(d) >= nz:
                    return zero
                if d == 0:
                    return z_out[it, which, rows, :]
                value = z_in[it, (nz - d - 1) % nz if d > 0 else -d - 1, which, rows, :]
                inside = jnp.logical_and(iz + d >= 0, iz + d < nz)
                return jnp.where(inside, value, 0.0)

            own_up = own_dn = zero
            for d in range(-(nz - 1), nz):
                j = iz + d
                inside = jnp.logical_and(j >= 0, j < nz)
                under, over = piece(d - 1, 3), piece(d + 1, 2)
                upt = piece(d, 0) + near * under - over
                dnt = piece(d, 1) + under - near * over
                if d == 0:
                    own_up, own_dn = upt, dnt
                    delta_low, delta_high = under, over
                elif d < 0:
                    below = below + jnp.where(inside, power(n * (-1 - d)) * upt, 0.0)
                else:
                    above = above + jnp.where(inside, power(n * (d - 1)) * dnt, 0.0)
                to_low = to_low + jnp.where(inside, power(n * j + 1) * dnt, 0.0)
                to_high = to_high + jnp.where(inside, power(n * (nz - 1 - j) + 1) * upt, 0.0)
            q = power(n * nz + 1)
            scale = kappa / (1.0 - q * q)
            alpha = kappa * below + (q * to_high - to_low) * scale * power(n * iz)
            beta = kappa * above + (q * to_low - to_high) * scale * power(n * (nz - 1 - iz))
            far = power(n + 1)
            bounds[2, rows, :] = kappa * mu * own_dn + alpha + beta * far
            bounds[3, rows, :] = kappa * mu * own_up + beta + alpha * far
            alpha = alpha + kappa * delta_low * inv
            beta = beta - kappa * delta_high * inv
            bounds[0, rows, :] = kappa * mu * z_out[it, 0, rows, :] + beta
            bounds[1, rows, :] = alpha * power(n)

        strips(body, h)

    def pass_two(it, h):
        last = it == ITERS - 1

        def body(r0):
            rows = pl.ds(r0, ROWS)
            mu, inv = mu_s[rows, :], planes[2, rows, :]
            half = 0.5 * mass[rows, :]
            zero = jnp.zeros((ROWS, nj), jnp.float32)

            def finish(k, above, below, packs):
                p = press[k, rows, :] - half * (above - below)
                if last:
                    press[k, rows, :] = p
                    return packs
                pp[k, pl.ds(PAD + r0, ROWS), :] = p
                return packed(p, k, packs)

            def steps(ks, carry):
                x, h, older, newer, packs = carry
                for k in ks:
                    x = mu * x + vert[k, rows, :]
                    v = x + h
                    h = h * inv
                    vert[k, rows, :] = v
                    geo[k, rows, :] = geo[k, rows, :] + 0.5 * v
                    if not (isinstance(k, int) and k == n - 1):
                        packs = finish(k + 1, older, v, packs)
                    older, newer = newer, v
                return x, h, older, newer, packs

            top = bounds[3, rows, :]
            carry = (bounds[0, rows, :], bounds[1, rows, :], zero, top, (zero, zero))
            carry = steps([n - 1 - e for e in range(unroll)], carry)

            def group(q, carry):
                return steps([n - 1 - q * unroll - e for e in range(unroll)], carry)

            _, _, older, newer, packs = lax.fori_loop(1, n // unroll, group, carry)
            packs = finish(0, older, bounds[2, rows, :], packs)
            if not last:
                for t in range(2):
                    col_out[it + 1, t, rows, :] = packs[t]

        strips(body, h)

    def winds():
        def body(r0):
            rows = pl.ds(r0, ROWS)
            left = col_in[0, 0, rows, :]
            right = col_in[0, 1, rows, :]
            for it in range(1, ITERS):
                left = left + col_in[it, 0, rows, :]
                right = right + col_in[it, 1, rows, :]

            ends = merged(left, right, 1)

            def group(q, carry):
                for e in range(unroll):
                    k = q * unroll + e
                    end = roll(ends[e % 2], nj - 2 - 2 * k)
                    at = pl.ds(PAD + r0, ROWS)
                    p = psum[k, at, :]
                    east[k, rows, :] = up[k, at, :] - 0.25 * (
                        psum[k, pl.ds(PAD + r0 + 1, ROWS), :] - psum[k, pl.ds(PAD + r0 - 1, ROWS), :])
                    low = jnp.where(lane < 1, end, roll(p, 1))
                    high = jnp.where(lane >= nj - 1, end, roll(p, nj - 1))
                    north[k, rows, :] = north[k, rows, :] - 0.25 * (high - low)
                return carry

            lax.fori_loop(0, n // unroll, group, 0)

        strips(body)

    for it in range(ITERS):
        if it > 0:
            recv_rows(it, pp)

        @pl.loop(0, PARTS)
        def _(h, it=it):
            if it > 0:
                for t in range(2):
                    col_copy(it, t, h).wait()
            pass_one(it, h)
            for d in range(1, nz):
                z_copy(it, d, h).start()

        if it == ITERS - 1:
            for t, at in ((0, PAD - 2), (1, PAD + ni)):
                total = row_in[0, t]
                for slot in range(1, ITERS):
                    total = total + row_in[slot, t]
                psum[:, at : at + 2, :] = total
            winds()

        @pl.loop(0, PARTS)
        def _(h, it=it):
            for d in range(1, nz):
                z_copy(it, d, h).wait()
            interface(it, h)
            pass_two(it, h)
            if it < ITERS - 1:
                for t in range(2):
                    col_copy(it + 1, t, h).start()

        if it < ITERS - 1:
            send_rows(it + 1, pp)


def local(sizes, east, north, vert, geo, press, mass):
    n, ni, nj = east.shape
    nz = sizes[2]
    f32 = jnp.float32
    slots = ITERS + 1
    field = pltpu.VMEM((n, ni, nj), f32)
    padded = pltpu.VMEM((n, ni + 2 * PAD, nj), f32)
    plane = pltpu.VMEM((ni, nj), f32)
    return pl.pallas_call(
        functools.partial(kernel, n, ni, nj, sizes),
        out_shape=[pltpu.VMEM((n, ni, nj), f32)] * 5,
        in_specs=[pl.BlockSpec(memory_space=pl.ANY)] * 5 + [pl.BlockSpec(memory_space=pltpu.VMEM)],
        out_specs=[pl.BlockSpec(memory_space=pltpu.VMEM)] * 5,
        scratch_shapes=[
            padded, padded, padded, field, plane, plane,
            pltpu.VMEM((3, ni, nj), f32),
            pltpu.VMEM((4, ni, nj), f32),
            pltpu.VMEM((slots, 2, n, 2, nj), f32),
            pltpu.VMEM((slots, 2, n, 2, nj), f32),
            pltpu.VMEM((slots, 2, ni, nj), f32),
            pltpu.VMEM((slots, 2, ni, nj), f32),
            pltpu.VMEM((ITERS, 4, ni, nj), f32),
            pltpu.VMEM((ITERS, nz - 1, 4, ni, nj), f32),
            pltpu.SemaphoreType.DMA((5,)),
            pltpu.SemaphoreType.DMA((slots, 2)),
            pltpu.SemaphoreType.DMA((slots, 2)),
            pltpu.SemaphoreType.DMA((slots, 2, PARTS)),
            pltpu.SemaphoreType.DMA((slots, 2, PARTS)),
            pltpu.SemaphoreType.DMA((ITERS, nz - 1, PARTS)),
            pltpu.SemaphoreType.DMA((ITERS, nz - 1, PARTS)),
        ],
        compiler_params=pltpu.CompilerParams(
            collective_id=0, has_side_effects=True, vmem_limit_bytes=40 * 1024 * 1024),
    )(east, north, vert, geo, press, mass)


FRONT = 3


def paired(n, ni, nj, sizes, east_in, north_in, vert_in, geo_in, press_in, mass_in,
           rhs, star, geo, coef, p0, up, north, edge, faces,
           p1, p2, dvg, head, side, mass, con, pack,
           row_out, row_in, col_out, col_in, z_out, z_in,
           load_sem, row_send, row_recv, col_send, col_recv, z_send, z_recv):
    nx, ny, _ = sizes
    per = nj // 4
    count = ni // ROWS
    press = (p0, p1, p2)
    ix, iy, iz = lax.axis_index("gx"), lax.axis_index("gy"), lax.axis_index("gz")
    xs = (lax.rem(ix + nx - 1, nx), lax.rem(ix + 1, nx))
    ys = (lax.rem(iy + ny - 1, ny), lax.rem(iy + 1, ny))
    flip = (1 - 2 * iz).astype(jnp.float32)
    inner = pl.ds(PAD, ni)

    fields = (
        (press_in, p0.at[:, inner, :]), (north_in, north), (east_in, up.at[:, inner, :]),
        (vert_in, head), (geo_in, geo))
    mass_load = pltpu.make_async_copy(mass_in, mass, load_sem.at[5])
    mass_load.start()
    for e, (src, dst) in enumerate(fields):
        @pl.loop(0, n)
        def _(m, e=e, src=src, dst=dst):
            k = iz * (n - 1) + (1 - 2 * iz) * m
            pltpu.make_async_copy(src.at[k], dst.at[m], load_sem.at[e]).start()

    def loaded(e):
        pltpu.make_async_copy(fields[e][0], fields[e][1], load_sem.at[e]).wait()

    barrier = pltpu.get_barrier_semaphore()
    for t in range(2):
        pl.semaphore_signal(barrier, inc=1, device_id={"gx": xs[t]})
        pl.semaphore_signal(barrier, inc=1, device_id={"gy": ys[t]})
    pl.semaphore_signal(barrier, inc=1, device_id={"gz": 1 - iz})

    def row_copy(it, t):
        return pltpu.make_async_remote_copy(
            src_ref=row_out.at[it, t], dst_ref=row_in.at[it, 1 - t],
            send_sem=row_send.at[it, t], recv_sem=row_recv.at[it, 1 - t],
            device_id={"gx": xs[t]})

    def rows_of(s):
        return pl.ds(pl.multiple_of(s * ROWS, ROWS), ROWS)

    def col_copy(it, t, s):
        return pltpu.make_async_remote_copy(
            src_ref=col_out.at[it, t, rows_of(s), :], dst_ref=col_in.at[it, 1 - t, rows_of(s), :],
            send_sem=col_send.at[it, t, s], recv_sem=col_recv.at[it, 1 - t, s],
            device_id={"gy": ys[t]})

    def z_copy(it, s):
        return pltpu.make_async_remote_copy(
            src_ref=z_out.at[it, :, rows_of(s), :], dst_ref=z_in.at[it, :, rows_of(s), :],
            send_sem=z_send.at[it, s], recv_sem=z_recv.at[it, s],
            device_id={"gz": 1 - iz})

    lane = lax.broadcasted_iota(jnp.int32, (ROWS, nj), 1)
    quad, part = lane // 4, lane % 4
    zero = jnp.zeros((ROWS, nj), jnp.float32)

    def packed(value, m, packs):
        turned = roll(value, 4 * (m % per) + 2)
        b = m // per
        return tuple(jnp.where(quad == m % per, turned, packs[c]) if c == b else packs[c] for c in range(2))

    def outgoing(it, rows, packs):
        a, b = packs
        col_out[it, 0, rows, :] = jnp.where(part >= 2, a, roll(b, -2))
        col_out[it, 1, rows, :] = jnp.where(part < 2, a, roll(b, 2))

    def incoming(left, right):
        return (jnp.where(part < 2, roll(right, -2), roll(left, 2)),
                jnp.where(part < 2, right, left))

    def sides(value, ends, m, width):
        end = roll(ends[m // per], nj - 2 - 4 * (m % per))
        low = jnp.where(lane < width, end, roll(value, width))
        high = jnp.where(lane >= nj - width, end, roll(value, nj - width))
        return low, high

    loaded(0)
    loaded(1)

    @pl.loop(0, count)
    def _(s):
        rows = rows_of(s)
        at = pl.ds(PAD + pl.multiple_of(s * ROWS, ROWS), ROWS)
        pk, vk = (zero, zero), (zero, zero)
        for m in range(n):
            pk = packed(p0[m, at, :], m, pk)
            vk = packed(north[m, rows, :], m, vk)
        packs = tuple(
            a + jnp.where(part == 0, 4.0 * roll(v, -1), jnp.where(part == 3, -4.0 * roll(v, 1), 0.0))
            for a, v in zip(pk, vk))
        outgoing(0, rows, packs)

    loaded(2)
    up[:, :PAD, :] = jnp.zeros((n, PAD, nj), jnp.float32)
    up[:, PAD + ni :, :] = jnp.zeros((n, PAD, nj), jnp.float32)
    row_out[0, 0] = p0[:, PAD : PAD + 2, :] - 4.0 * up[:, PAD - 1 : PAD + 1, :]
    row_out[0, 1] = p0[:, PAD + ni - 2 : PAD + ni, :] + 4.0 * up[:, PAD + ni - 1 : PAD + ni + 1, :]

    pl.semaphore_wait(barrier, 5)

    @pl.loop(0, count)
    def _(s):
        for t in range(2):
            col_copy(0, t, s).start()

    for t in range(2):
        row_copy(0, t).start()

    mass_load.wait()
    inverse = 1.0 / (STIFF * mass[...])
    con[0] = 1.25 * inverse
    con[1] = 0.25 * inverse
    base = 2.0 + inverse

    def pivot(m, a):
        a = 1.0 / (base - a)
        coef[m] = a
        return a

    last = lax.fori_loop(0, n, pivot, jnp.zeros((ni, nj), jnp.float32))
    con[2] = last / (1.0 - last * last)

    @pl.loop(0, count)
    def _(s):
        rows = rows_of(s)
        r0 = PAD + pl.multiple_of(s * ROWS, ROWS)
        strong = 0.2 * mass[rows, :]
        for m in range(n):
            v = north[m, rows, :]
            low = jnp.where(lane < 1, 0.0, roll(v, 1))
            high = jnp.where(lane >= nj - 1, 0.0, roll(v, nj - 1))
            dvg[m, rows, :] = strong * (
                (up[m, pl.ds(r0 + 1, ROWS), :] - up[m, pl.ds(r0 - 1, ROWS), :]) + (high - low))

    loaded(3)
    loaded(4)

    @pl.loop(0, count)
    def _(s):
        rows = rows_of(s)
        for m in range(n):
            g = (0.5 * flip) * geo[m, rows, :]
            geo[m, rows, :] = g
            head[m, rows, :] = flip * head[m, rows, :] + g

    def lateral(it, s):
        rows = rows_of(s)
        at = pl.ds(PAD + pl.multiple_of(s * ROWS, ROWS), ROWS)
        ends = incoming(col_in[it, 0, rows, :], col_in[it, 1, rows, :])

        def level(m):
            low, high = sides(press[it][m, at, :], ends, m, 2)
            side[m] = low + high

        return level

    def forward(it, s):
        rows = rows_of(s)
        r0 = PAD + pl.multiple_of(s * ROWS, ROWS)
        at = pl.ds(r0, ROWS)
        weak = 0.05 * mass[rows, :]
        four = 4.0 * weak
        state = {"older": zero, "newer": None, "g": None}

        def close(m, above):
            g = head[m, rows, :] - (above - state["older"])
            if m > 0:
                g = g + coef[m - 1, rows, :] * state["g"]
            rhs[m, rows, :] = g
            state["g"] = g

        def level(m):
            ref = press[it]
            p = ref[m, at, :]
            total = (ref[m, pl.ds(r0 + 2, ROWS), :] + ref[m, pl.ds(r0 - 2, ROWS), :]) + side[m]
            d = (dvg[m, rows, :] + four * p) - weak * total
            if it < ITERS - 1:
                dvg[m, rows, :] = d
            else:
                p0[m, at, :] = (p0[m, at, :] + p1[m, at, :]) + p
            ps = p - d
            star[m, rows, :] = ps
            if m > 0:
                close(m - 1, ps)
                state["older"] = state["newer"]
            state["newer"] = ps

        def finish():
            close(n - 1, zero)
            z_out[it, 0, rows, :] = state["g"]
            z_out[it, 1, rows, :] = state["newer"]
            z_copy(it, s).start()

        return level, finish

    def col_wait(it, s):
        for t in range(2):
            col_copy(it, t, s).wait()

    def row_wait(it):
        for t in range(2):
            row_copy(it, t).wait()
        press[it][:, PAD - 2 : PAD, :] = row_in[it, 0]
        press[it][:, PAD + ni : PAD + ni + 2, :] = row_in[it, 1]

    def pass_one(it):
        col_wait(it, 1)
        level = lateral(it, 1)
        for m in range(n):
            level(m)

        @pl.loop(1, count)
        def _(s):
            @pl.when(s == count - 1)
            def _():
                row_wait(it)

            after = lax.rem(s + 1, count)
            col_wait(it, after)
            level, finish = forward(it, s)
            ahead = lateral(it, after)
            for m in range(n):
                level(m)
                ahead(m)
            finish()

        level, finish = forward(it, 0)
        for m in range(n):
            level(m)
        finish()

    def interface(it, s):
        rows = rows_of(s)
        z_copy(it, s).wait()
        a, w = coef[n - 1, rows, :], con[2, rows, :]
        mine = z_out[it, 0, rows, :] - z_in[it, 1, rows, :]
        other = z_in[it, 0, rows, :] - z_out[it, 1, rows, :]
        z = w * (mine - a * other)
        return z, a * (z - other)

    def backward(it, s):
        rows = rows_of(s)
        at = pl.ds(PAD + pl.multiple_of(s * ROWS, ROWS), ROWS)
        near, far = con[0, rows, :], con[1, rows, :]
        z, above = interface(it, s)
        packs = (zero, zero)
        for m in range(n - 1, -1, -1):
            g = geo[m, rows, :]
            head[m, rows, :] = near * z + g
            geo[m, rows, :] = far * z + g
            below = coef[m - 1, rows, :] * (rhs[m - 1, rows, :] + z) if m > 0 else zero
            p = star[m, rows, :] - (0.5 / STIFF) * (above - below)
            press[it + 1][m, at, :] = p
            packs = packed(p, m, packs)
            above, z = z, below
        outgoing(it + 1, rows, packs)
        for t in range(2):
            col_copy(it + 1, t, s).start()

    def pass_two(it):
        @pl.loop(0, count)
        def _(t):
            s = jnp.where(t < FRONT, t + 1, jnp.where(t == FRONT, count - 1, jnp.where(t == FRONT + 1, 0, t - 1)))
            backward(it, s)

            @pl.when(t == FRONT)
            def _():
                row_out[it + 1, 1] = press[it + 1][:, PAD + ni - 2 : PAD + ni, :]
                row_copy(it + 1, 1).start()

            @pl.when(t == FRONT + 1)
            def _():
                row_out[it + 1, 0] = press[it + 1][:, PAD : PAD + 2, :]
                row_copy(it + 1, 0).start()

    for it in range(ITERS):
        pass_one(it)
        if it < ITERS - 1:
            pass_two(it)

    for t, at in ((0, PAD - 2), (1, PAD + ni)):
        p0[:, at : at + 2, :] = (row_in[0, t] + row_in[1, t]) + row_in[2, t]

    def closing(s):
        rows = rows_of(s)
        left = (col_in[0, 0, rows, :] + col_in[1, 0, rows, :]) + col_in[2, 0, rows, :]
        right = (col_in[0, 1, rows, :] + col_in[1, 1, rows, :]) + col_in[2, 1, rows, :]
        edge[0, rows, :] = jnp.where(part == 1, roll(right, -1), roll(left, 1))
        edge[1, rows, :] = jnp.where(part == 1, roll(right, 1), roll(left, -1))

    @pl.loop(0, count)
    def _(s):
        closing(s)

    @pl.loop(0, count)
    def _(t):
        s = lax.rem(t + 1, count)
        faces[0, rows_of(s), :], faces[1, rows_of(s), :] = interface(ITERS - 1, s)


def finale(n, ni, nj, rhs, star, geo, coef, psum, up, north, edge, faces, mass,
           east_out, north_out, vert_out, geo_out, press_out,
           east_s, north_s, vert_s, geo_s, press_s, sem):
    per = nj // 4
    count = ni // ROWS
    iz = lax.axis_index("gz")
    flip = (1 - 2 * iz).astype(jnp.float32)
    lane = lax.broadcasted_iota(jnp.int32, (ROWS, nj), 1)

    def store(e, src, dst, rows):
        return pltpu.make_async_copy(src.at[:, rows, :], dst.at[:, rows, :], sem.at[e])

    outs = ((east_s, east_out), (north_s, north_out), (vert_s, vert_out), (geo_s, geo_out), (press_s, press_out))

    def level_of(m):
        return iz * (n - 1) + (1 - 2 * iz) * m

    @pl.loop(0, count)
    def _(s):
        rows = pl.ds(pl.multiple_of(s * ROWS, ROWS), ROWS)
        v_of = flip / (STIFF * mass[rows, :])
        half = 0.5 * v_of
        twice = 2.0 * flip
        z, above = faces[0, rows, :], faces[1, rows, :]
        for m in range(n - 1, -1, -1):
            k = level_of(m)
            vert_s[k, rows, :] = v_of * z
            geo_s[k, rows, :] = twice * geo[m, rows, :] + half * z
            below = coef[m - 1, rows, :] * (rhs[m - 1, rows, :] + z) if m > 0 else jnp.zeros_like(z)
            press_s[k, rows, :] = star[m, rows, :] - (0.5 / STIFF) * (above - below)
            above, z = z, below
        for e in (2, 3, 4):
            store(e, *outs[e], rows).start()

    @pl.loop(0, count)
    def _(s):
        rows = pl.ds(pl.multiple_of(s * ROWS, ROWS), ROWS)
        r0 = PAD + pl.multiple_of(s * ROWS, ROWS)
        ends = (edge[0, rows, :], edge[1, rows, :])
        for m in range(n):
            k = level_of(m)
            p = psum[m, pl.ds(r0, ROWS), :]
            end = roll(ends[m // per], nj - 2 - 4 * (m % per))
            low = jnp.where(lane < 1, end, roll(p, 1))
            high = jnp.where(lane >= nj - 1, end, roll(p, nj - 1))
            north_s[k, rows, :] = north[m, rows, :] - 0.25 * (high - low)
            east_s[k, rows, :] = up[m, pl.ds(r0, ROWS), :] - 0.25 * (
                psum[m, pl.ds(r0 + 1, ROWS), :] - psum[m, pl.ds(r0 - 1, ROWS), :])
        for e in (0, 1):
            store(e, *outs[e], rows).start()

    for e in range(5):
        pltpu.make_async_copy(outs[e][0], outs[e][1], sem.at[e]).wait()


def pair(sizes, east, north, vert, geo, press, mass):
    n, ni, nj = east.shape
    f32 = jnp.float32
    count = ni // ROWS
    shape = (n, ni, nj)
    padded = (n, ni + 2 * PAD, nj)
    kept = [shape, shape, shape, shape, padded, padded, shape, (2, ni, nj), (2, ni, nj)]
    vmem = pl.BlockSpec(memory_space=pltpu.VMEM)
    state = pl.pallas_call(
        functools.partial(paired, n, ni, nj, sizes),
        out_shape=[pltpu.VMEM(s, f32) for s in kept],
        in_specs=[pl.BlockSpec(memory_space=pl.ANY)] * 6,
        out_specs=[vmem] * len(kept),
        scratch_shapes=[
            pltpu.VMEM(padded, f32), pltpu.VMEM(padded, f32), pltpu.VMEM(shape, f32), pltpu.VMEM(shape, f32),
            pltpu.VMEM((n, ROWS, nj), f32),
            pltpu.VMEM((ni, nj), f32),
            pltpu.VMEM((3, ni, nj), f32),
            pltpu.VMEM((2, ni, nj), f32),
            pltpu.VMEM((ITERS, 2, n, 2, nj), f32),
            pltpu.VMEM((ITERS, 2, n, 2, nj), f32),
            pltpu.VMEM((ITERS, 2, ni, nj), f32),
            pltpu.VMEM((ITERS, 2, ni, nj), f32),
            pltpu.VMEM((ITERS, 2, ni, nj), f32),
            pltpu.VMEM((ITERS, 2, ni, nj), f32),
            pltpu.SemaphoreType.DMA((6,)),
            pltpu.SemaphoreType.DMA((ITERS, 2)),
            pltpu.SemaphoreType.DMA((ITERS, 2)),
            pltpu.SemaphoreType.DMA((ITERS, 2, count)),
            pltpu.SemaphoreType.DMA((ITERS, 2, count)),
            pltpu.SemaphoreType.DMA((ITERS, count)),
            pltpu.SemaphoreType.DMA((ITERS, count)),
        ],
        compiler_params=pltpu.CompilerParams(
            collective_id=0, has_side_effects=True, vmem_limit_bytes=25 * 1024 * 1024),
    )(east, north, vert, geo, press, mass)
    return pl.pallas_call(
        functools.partial(finale, n, ni, nj),
        out_shape=[jax.ShapeDtypeStruct(shape, f32)] * 5,
        in_specs=[vmem] * (len(kept) + 1),
        out_specs=[pl.BlockSpec(memory_space=pl.ANY)] * 5,
        scratch_shapes=[pltpu.VMEM(shape, f32)] * 5 + [pltpu.SemaphoreType.DMA((5,))],
        compiler_params=pltpu.CompilerParams(vmem_limit_bytes=18 * 1024 * 1024),
    )(*state, mass)


def solution(mesh):
    sizes = (mesh.shape["gx"], mesh.shape["gy"], mesh.shape["gz"])
    cube = P("gz", "gx", "gy")

    def body(east, *rest):
        n, ni, nj = east.shape
        fits = sizes[2] == 2 and n <= nj // 2 and ni // ROWS > FRONT + 2 and ITERS == 3
        return (pair if fits else local)(sizes, east, *rest)

    return jax.shard_map(
        body, mesh=mesh,
        in_specs=(cube,) * 5 + (P("gx", "gy"),), out_specs=(cube,) * 5, check_vma=False)
```

```python
import functools

import jax
import jax.numpy as jnp
from jax import lax
from jax.experimental import pallas as pl
from jax.experimental.pallas import tpu as pltpu
from jax.sharding import PartitionSpec as P

ITERS = 3
STIFF = 30.0
PAD = 8
ROWS = 16
PARTS = 2
UNROLL = 24


def roll(value, shift):
    if isinstance(shift, int):
        shift = shift % value.shape[1]
    return pltpu.roll(value, shift, 1)


def kernel(n, ni, nj, sizes, east_in, north_in, vert_in, geo_in, press_in, mass,
           east, north, vert, geo, press,
           pp, up, psum, dvg, mu_s, c_s, planes, bounds,
           row_out, row_in, col_out, col_in, z_out, z_in,
           load_sem, row_send, row_recv, col_send, col_recv, z_send, z_recv):
    nx, ny, nz = sizes
    unroll = max(u for u in range(2, UNROLL + 1) if n % u == 0 and u % 2 == 0)
    ix, iy, iz = lax.axis_index("gx"), lax.axis_index("gy"), lax.axis_index("gz")
    xs = (lax.rem(ix + nx - 1, nx), lax.rem(ix + 1, nx))
    ys = (lax.rem(iy + ny - 1, ny), lax.rem(iy + 1, ny))

    loads = [
        pltpu.make_async_copy(press_in, pp.at[:, pl.ds(PAD, ni), :], load_sem.at[0]),
        pltpu.make_async_copy(east_in, up.at[:, pl.ds(PAD, ni), :], load_sem.at[1]),
        pltpu.make_async_copy(north_in, north, load_sem.at[2]),
        pltpu.make_async_copy(vert_in, vert, load_sem.at[3]),
        pltpu.make_async_copy(geo_in, geo, load_sem.at[4]),
    ]
    for load in loads:
        load.start()

    barrier = pltpu.get_barrier_semaphore()
    for t in range(2):
        pl.semaphore_signal(barrier, inc=1, device_id={"gx": xs[t]})
        pl.semaphore_signal(barrier, inc=1, device_id={"gy": ys[t]})
    for d in range(1, nz):
        pl.semaphore_signal(barrier, inc=1, device_id={"gz": lax.rem(iz + d, nz)})
    pl.semaphore_wait(barrier, 4 + nz - 1)

    def row_copy(slot, t):
        return pltpu.make_async_remote_copy(
            src_ref=row_out.at[slot, t], dst_ref=row_in.at[slot, 1 - t],
            send_sem=row_send.at[slot, t], recv_sem=row_recv.at[slot, 1 - t],
            device_id={"gx": xs[t]})

    span = ni // PARTS

    def part_rows(h):
        return pl.ds(pl.multiple_of(h * span, span), span)

    def col_copy(slot, t, h):
        return pltpu.make_async_remote_copy(
            src_ref=col_out.at[slot, t, part_rows(h), :], dst_ref=col_in.at[slot, 1 - t, part_rows(h), :],
            send_sem=col_send.at[slot, t, h], recv_sem=col_recv.at[slot, 1 - t, h],
            device_id={"gy": ys[t]})

    def z_copy(slot, d, h):
        return pltpu.make_async_remote_copy(
            src_ref=z_out.at[slot, :, part_rows(h), :], dst_ref=z_in.at[slot, d - 1, :, part_rows(h), :],
            send_sem=z_send.at[slot, d - 1, h], recv_sem=z_recv.at[slot, d - 1, h],
            device_id={"gz": lax.rem(iz + d, nz)})

    lane = lax.broadcasted_iota(jnp.int32, (ROWS, nj), 1)
    pair = lane // 2

    def merged(left, right, width):
        left, right = roll(left, width), roll(right, nj - width)
        even = pair % 2 == 0
        return jnp.where(even, right, left), jnp.where(even, left, right)

    def send_rows(slot, ref):
        row_out[slot, 0] = ref[:, PAD : PAD + 2, :]
        row_out[slot, 1] = ref[:, PAD + ni - 2 : PAD + ni, :]
        for t in range(2):
            row_copy(slot, t).start()

    def recv_rows(slot, ref):
        for t in range(2):
            row_copy(slot, t).wait()
        ref[:, PAD - 2 : PAD, :] = row_in[slot, 0]
        ref[:, PAD + ni : PAD + ni + 2, :] = row_in[slot, 1]

    def packed(value, k, packs):
        turned = roll(value, 2 * k + 2)
        return (jnp.where(pair == k + 1, turned, packs[0]), jnp.where(pair == k, turned, packs[1]))

    def strips(body, h=None):
        count = (ni if h is None else span) // ROWS
        first = 0 if h is None else h * count

        @pl.loop(0, count)
        def _(s):
            body(pl.multiple_of((first + s) * ROWS, ROWS))

    def send_cols(slot, load_level):
        def body(r0):
            zero = jnp.zeros((ROWS, nj), jnp.float32)

            def group(q, packs):
                for e in range(unroll):
                    k = q * unroll + e
                    packs = packed(load_level(k, r0), k, packs)
                return packs

            packs = lax.fori_loop(0, n // unroll, group, (zero, zero))
            for t in range(2):
                col_out[slot, t, pl.ds(r0, ROWS), :] = packs[t]

        strips(body)
        for h in range(PARTS):
            for t in range(2):
                col_copy(slot, t, h).start()

    loads[0].wait()
    send_rows(0, pp)
    send_cols(0, lambda k, r0: pp[k, pl.ds(PAD + r0, ROWS), :])
    loads[1].wait()
    send_rows(ITERS, up)
    loads[2].wait()
    send_cols(ITERS, lambda k, r0: north[k, pl.ds(r0, ROWS), :])

    stiff = STIFF * mass[...]
    root = jnp.sqrt(1.0 + 4.0 * stiff)
    major = 0.5 * (1.0 + 2.0 * stiff + root)
    mu_s[...] = stiff / major
    c_s[...] = 1.0 / major
    planes[0] = jnp.log(stiff / major)
    planes[1] = major / root
    planes[2] = major / stiff

    recv_rows(0, pp)
    recv_rows(ITERS, up)
    for slot in (0, ITERS):
        for t in range(2):
            for h in range(PARTS):
                col_copy(slot, t, h).wait()
    loads[3].wait()
    loads[4].wait()

    def pass_one(it, h):
        def body(r0):
            rows = pl.ds(r0, ROWS)
            m, mu, c = mass[rows, :], mu_s[rows, :], c_s[rows, :]
            weak, strong = 0.05 * m, 0.2 * m
            left, right = col_in[it, 0, rows, :], col_in[it, 1, rows, :]
            ends = merged(left, right, 2)
            if it == 0:
                vends = merged(col_in[ITERS, 0, rows, :], col_in[ITERS, 1, rows, :], 1)

            def star(k, parity):
                end = roll(ends[parity], nj - 2 - 2 * k)
                at = pl.ds(PAD + r0, ROWS)
                p = pp[k, at, :]
                low = jnp.where(lane < 2, end, roll(p, 2))
                high = jnp.where(lane >= nj - 2, end, roll(p, nj - 2))
                total = (pp[k, pl.ds(PAD + r0 + 2, ROWS), :] + pp[k, pl.ds(PAD + r0 - 2, ROWS), :]) + (low + high) - 4.0 * p
                if it == 0:
                    v = north[k, rows, :]
                    vend = roll(vends[parity], nj - 2 - 2 * k)
                    vlow = jnp.where(lane < 1, vend, roll(v, 1))
                    vhigh = jnp.where(lane >= nj - 1, vend, roll(v, nj - 1))
                    d = strong * (up[k, pl.ds(PAD + r0 + 1, ROWS), :] - up[k, pl.ds(PAD + r0 - 1, ROWS), :] + (vhigh - vlow))
                    psum[k, at, :] = p
                else:
                    d = dvg[k, rows, :]
                    psum[k, at, :] = psum[k, at, :] + p
                d = d - weak * total
                if it < ITERS - 1:
                    dvg[k, rows, :] = d
                ps = p - d
                press[k, rows, :] = ps
                return ps

            def sweep(k, above, below, state):
                y, dn, weight = state
                f = c * (vert[k, rows, :] + 0.5 * geo[k, rows, :] - (above - below))
                y = mu * y + f
                vert[k, rows, :] = y
                return y, dn + weight * f, weight * mu

            def steps(ks, carry):
                older, newer, state = carry
                for e, k in enumerate(ks):
                    ps = star(k, e % 2)
                    if not (isinstance(k, int) and k == 0):
                        state = sweep(k - 1, ps, older, state)
                    older, newer = newer, ps
                return older, newer, state

            zero = jnp.zeros((ROWS, nj), jnp.float32)
            carry = (zero, zero, (zero, zero, zero + 1.0))
            carry = steps(range(unroll), carry)
            planes_lo = press[0, rows, :]

            def group(q, carry):
                return steps([q * unroll + e for e in range(unroll)], carry)

            older, newer, state = lax.fori_loop(1, n // unroll, group, carry)
            y, dn, _ = sweep(n - 1, zero, older, state)
            z_out[it, 0, rows, :] = y
            z_out[it, 1, rows, :] = dn
            z_out[it, 2, rows, :] = c * planes_lo
            z_out[it, 3, rows, :] = c * newer

        strips(body, h)

    def interface(it, h):
        def body(r0):
            rows = pl.ds(r0, ROWS)
            mu, logmu, kappa, inv = mu_s[rows, :], planes[0, rows, :], planes[1, rows, :], planes[2, rows, :]
            zero = jnp.zeros((ROWS, nj), jnp.float32)

            def power(m):
                if not isinstance(m, int):
                    m = jnp.maximum(m, 0).astype(jnp.float32)
                return jnp.exp(m * logmu)

            near = power(n - 1)
            below, above, to_low, to_high = zero, zero, zero, zero
            pieces = {}

            def piece(d, which):
                if abs(d) >= nz:
                    return zero
                if d == 0:
                    return z_out[it, which, rows, :]
                value = z_in[it, (nz - d - 1) % nz if d > 0 else -d - 1, which, rows, :]
                inside = jnp.logical_and(iz + d >= 0, iz + d < nz)
                return jnp.where(inside, value, 0.0)

            own_up = own_dn = zero
            for d in range(-(nz - 1), nz):
                j = iz + d
                inside = jnp.logical_and(j >= 0, j < nz)
                under, over = piece(d - 1, 3), piece(d + 1, 2)
                upt = piece(d, 0) + near * under - over
                dnt = piece(d, 1) + under - near * over
                if d == 0:
                    own_up, own_dn = upt, dnt
                    delta_low, delta_high = under, over
                elif d < 0:
                    below = below + jnp.where(inside, power(n * (-1 - d)) * upt, 0.0)
                else:
                    above = above + jnp.where(inside, power(n * (d - 1)) * dnt, 0.0)
                to_low = to_low + jnp.where(inside, power(n * j + 1) * dnt, 0.0)
                to_high = to_high + jnp.where(inside, power(n * (nz - 1 - j) + 1) * upt, 0.0)
            q = power(n * nz + 1)
            scale = kappa / (1.0 - q * q)
            alpha = kappa * below + (q * to_high - to_low) * scale * power(n * iz)
            beta = kappa * above + (q * to_low - to_high) * scale * power(n * (nz - 1 - iz))
            far = power(n + 1)
            bounds[2, rows, :] = kappa * mu * own_dn + alpha + beta * far
            bounds[3, rows, :] = kappa * mu * own_up + beta + alpha * far
            alpha = alpha + kappa * delta_low * inv
            beta = beta - kappa * delta_high * inv
            bounds[0, rows, :] = kappa * mu * z_out[it, 0, rows, :] + beta
            bounds[1, rows, :] = alpha * power(n)

        strips(body, h)

    def pass_two(it, h):
        last = it == ITERS - 1

        def body(r0):
            rows = pl.ds(r0, ROWS)
            mu, inv = mu_s[rows, :], planes[2, rows, :]
            half = 0.5 * mass[rows, :]
            zero = jnp.zeros((ROWS, nj), jnp.float32)

            def finish(k, above, below, packs):
                p = press[k, rows, :] - half * (above - below)
                if last:
                    press[k, rows, :] = p
                    return packs
                pp[k, pl.ds(PAD + r0, ROWS), :] = p
                return packed(p, k, packs)

            def steps(ks, carry):
                x, h, older, newer, packs = carry
                for k in ks:
                    x = mu * x + vert[k, rows, :]
                    v = x + h
                    h = h * inv
                    vert[k, rows, :] = v
                    geo[k, rows, :] = geo[k, rows, :] + 0.5 * v
                    if not (isinstance(k, int) and k == n - 1):
                        packs = finish(k + 1, older, v, packs)
                    older, newer = newer, v
                return x, h, older, newer, packs

            top = bounds[3, rows, :]
            carry = (bounds[0, rows, :], bounds[1, rows, :], zero, top, (zero, zero))
            carry = steps([n - 1 - e for e in range(unroll)], carry)

            def group(q, carry):
                return steps([n - 1 - q * unroll - e for e in range(unroll)], carry)

            _, _, older, newer, packs = lax.fori_loop(1, n // unroll, group, carry)
            packs = finish(0, older, bounds[2, rows, :], packs)
            if not last:
                for t in range(2):
                    col_out[it + 1, t, rows, :] = packs[t]

        strips(body, h)

    def winds():
        def body(r0):
            rows = pl.ds(r0, ROWS)
            left = col_in[0, 0, rows, :]
            right = col_in[0, 1, rows, :]
            for it in range(1, ITERS):
                left = left + col_in[it, 0, rows, :]
                right = right + col_in[it, 1, rows, :]

            ends = merged(left, right, 1)

            def group(q, carry):
                for e in range(unroll):
                    k = q * unroll + e
                    end = roll(ends[e % 2], nj - 2 - 2 * k)
                    at = pl.ds(PAD + r0, ROWS)
                    p = psum[k, at, :]
                    east[k, rows, :] = up[k, at, :] - 0.25 * (
                        psum[k, pl.ds(PAD + r0 + 1, ROWS), :] - psum[k, pl.ds(PAD + r0 - 1, ROWS), :])
                    low = jnp.where(lane < 1, end, roll(p, 1))
                    high = jnp.where(lane >= nj - 1, end, roll(p, nj - 1))
                    north[k, rows, :] = north[k, rows, :] - 0.25 * (high - low)
                return carry

            lax.fori_loop(0, n // unroll, group, 0)

        strips(body)

    for it in range(ITERS):
        if it > 0:
            recv_rows(it, pp)

        @pl.loop(0, PARTS)
        def _(h, it=it):
            if it > 0:
                for t in range(2):
                    col_copy(it, t, h).wait()
            pass_one(it, h)
            for d in range(1, nz):
                z_copy(it, d, h).start()

        if it == ITERS - 1:
            for t, at in ((0, PAD - 2), (1, PAD + ni)):
                total = row_in[0, t]
                for slot in range(1, ITERS):
                    total = total + row_in[slot, t]
                psum[:, at : at + 2, :] = total
            winds()

        @pl.loop(0, PARTS)
        def _(h, it=it):
            for d in range(1, nz):
                z_copy(it, d, h).wait()
            interface(it, h)
            pass_two(it, h)
            if it < ITERS - 1:
                for t in range(2):
                    col_copy(it + 1, t, h).start()

        if it < ITERS - 1:
            send_rows(it + 1, pp)


def local(sizes, east, north, vert, geo, press, mass):
    n, ni, nj = east.shape
    nz = sizes[2]
    f32 = jnp.float32
    slots = ITERS + 1
    field = pltpu.VMEM((n, ni, nj), f32)
    padded = pltpu.VMEM((n, ni + 2 * PAD, nj), f32)
    plane = pltpu.VMEM((ni, nj), f32)
    return pl.pallas_call(
        functools.partial(kernel, n, ni, nj, sizes),
        out_shape=[pltpu.VMEM((n, ni, nj), f32)] * 5,
        in_specs=[pl.BlockSpec(memory_space=pl.ANY)] * 5 + [pl.BlockSpec(memory_space=pltpu.VMEM)],
        out_specs=[pl.BlockSpec(memory_space=pltpu.VMEM)] * 5,
        scratch_shapes=[
            padded, padded, padded, field, plane, plane,
            pltpu.VMEM((3, ni, nj), f32),
            pltpu.VMEM((4, ni, nj), f32),
            pltpu.VMEM((slots, 2, n, 2, nj), f32),
            pltpu.VMEM((slots, 2, n, 2, nj), f32),
            pltpu.VMEM((slots, 2, ni, nj), f32),
            pltpu.VMEM((slots, 2, ni, nj), f32),
            pltpu.VMEM((ITERS, 4, ni, nj), f32),
            pltpu.VMEM((ITERS, nz - 1, 4, ni, nj), f32),
            pltpu.SemaphoreType.DMA((5,)),
            pltpu.SemaphoreType.DMA((slots, 2)),
            pltpu.SemaphoreType.DMA((slots, 2)),
            pltpu.SemaphoreType.DMA((slots, 2, PARTS)),
            pltpu.SemaphoreType.DMA((slots, 2, PARTS)),
            pltpu.SemaphoreType.DMA((ITERS, nz - 1, PARTS)),
            pltpu.SemaphoreType.DMA((ITERS, nz - 1, PARTS)),
        ],
        compiler_params=pltpu.CompilerParams(
            collective_id=0, has_side_effects=True, vmem_limit_bytes=40 * 1024 * 1024),
    )(east, north, vert, geo, press, mass)


FRONT = 3
WIDE = 32


def paired(n, ni, nj, sizes, east_in, north_in, vert_in, geo_in, press_in, mass_in,
           rhs, star, geo, coef, p0, up, north, edge, faces,
           p1, p2, dvg, head, turned, side, mass, con, packs_p, packs_v,
           row_out, row_in, col_out, col_in, z_out, z_in,
           load_sem, row_send, row_recv, col_send, col_recv, z_send, z_recv):
    nx, ny, _ = sizes
    per = nj // 4
    count = ni // ROWS
    press = (p0, p1, p2)
    ix, iy, iz = lax.axis_index("gx"), lax.axis_index("gy"), lax.axis_index("gz")
    xs = (lax.rem(ix + nx - 1, nx), lax.rem(ix + 1, nx))
    ys = (lax.rem(iy + ny - 1, ny), lax.rem(iy + 1, ny))
    flip = (1 - 2 * iz).astype(jnp.float32)
    inner = pl.ds(PAD, ni)

    fields = (
        (press_in, p0.at[:, inner, :]), (north_in, north), (east_in, up.at[:, inner, :]),
        (vert_in, head), (geo_in, geo))
    mass_load = pltpu.make_async_copy(mass_in, mass, load_sem.at[5])
    mass_load.start()
    for e, (src, dst) in enumerate(fields):
        @pl.loop(0, n)
        def _(m, e=e, src=src, dst=dst):
            k = iz * (n - 1) + (1 - 2 * iz) * m
            pltpu.make_async_copy(src.at[k], dst.at[m], load_sem.at[e]).start()

    def loaded(e):
        pltpu.make_async_copy(fields[e][0], fields[e][1], load_sem.at[e]).wait()

    barrier = pltpu.get_barrier_semaphore()
    for t in range(2):
        pl.semaphore_signal(barrier, inc=1, device_id={"gx": xs[t]})
        pl.semaphore_signal(barrier, inc=1, device_id={"gy": ys[t]})
    pl.semaphore_signal(barrier, inc=1, device_id={"gz": 1 - iz})

    def row_copy(it, t):
        return pltpu.make_async_remote_copy(
            src_ref=row_out.at[it, t], dst_ref=row_in.at[it, 1 - t],
            send_sem=row_send.at[it, t], recv_sem=row_recv.at[it, 1 - t],
            device_id={"gx": xs[t]})

    def rows_of(s):
        return pl.ds(pl.multiple_of(s * ROWS, ROWS), ROWS)

    def col_copy(it, t, s):
        return pltpu.make_async_remote_copy(
            src_ref=col_out.at[it, t, rows_of(s), :], dst_ref=col_in.at[it, 1 - t, rows_of(s), :],
            send_sem=col_send.at[it, t, s], recv_sem=col_recv.at[it, 1 - t, s],
            device_id={"gy": ys[t]})

    def z_copy(it, s):
        return pltpu.make_async_remote_copy(
            src_ref=z_out.at[it, :, rows_of(s), :], dst_ref=z_in.at[it, :, rows_of(s), :],
            send_sem=z_send.at[it, s], recv_sem=z_recv.at[it, s],
            device_id={"gz": 1 - iz})

    lane = lax.broadcasted_iota(jnp.int32, (ROWS, nj), 1)
    part, couple = lane % 4, lane // 2
    zero = jnp.zeros((ROWS, nj), jnp.float32)

    def placed(quad, value, m, packs):
        b = m // per
        return tuple(jnp.where(quad == m % per, value, packs[c]) if c == b else packs[c] for c in range(2))

    def outgoing(it, rows, packs):
        a, b = packs
        col_out[it, 0, rows, :] = jnp.where(part >= 2, a, roll(b, -2))
        col_out[it, 1, rows, :] = jnp.where(part < 2, a, roll(b, 2))

    def incoming(left, right):
        return (jnp.where(part < 2, left, right),
                jnp.where(part < 2, roll(left, -2), roll(right, 2)))

    def gather(ref, pad, packs, keep):
        quad = lax.broadcasted_iota(jnp.int32, (WIDE, nj), 1) // 4

        @pl.loop(0, ni // WIDE)
        def _(s):
            r0 = pl.multiple_of(s * WIDE, WIDE)
            rows = pl.ds(r0, WIDE)
            got = (jnp.zeros((WIDE, nj), jnp.float32),) * 2
            for m in range(n):
                value = roll(ref[m, pl.ds(pad + r0, WIDE), :], 4 * (m % per) + 2)
                if keep:
                    turned[m, rows, :] = value
                got = placed(quad, value, m, got)
            packs[0, rows, :], packs[1, rows, :] = got

    loaded(0)
    gather(p0, PAD, packs_p, True)
    loaded(1)
    gather(north, 0, packs_v, False)

    @pl.loop(0, count)
    def _(s):
        rows = rows_of(s)
        packs = []
        for c in range(2):
            v = packs_v[c, rows, :]
            packs.append(packs_p[c, rows, :] + jnp.where(
                part == 0, 4.0 * roll(v, -1), jnp.where(part == 3, -4.0 * roll(v, 1), 0.0)))
        outgoing(0, rows, packs)

    pl.semaphore_wait(barrier, 5)

    @pl.loop(0, count)
    def _(s):
        for t in range(2):
            col_copy(0, t, s).start()

    loaded(2)
    up[:, :PAD, :] = jnp.zeros((n, PAD, nj), jnp.float32)
    up[:, PAD + ni :, :] = jnp.zeros((n, PAD, nj), jnp.float32)
    row_out[0, 0] = p0[:, PAD : PAD + 2, :] - 4.0 * up[:, PAD - 1 : PAD + 1, :]
    row_out[0, 1] = p0[:, PAD + ni - 2 : PAD + ni, :] + 4.0 * up[:, PAD + ni - 1 : PAD + ni + 1, :]
    for t in range(2):
        row_copy(0, t).start()

    mass_load.wait()
    inverse = 1.0 / (STIFF * mass[...])
    con[0] = 1.25 * inverse
    con[1] = 0.25 * inverse
    base = 2.0 + inverse

    def pivot(m, a):
        a = 1.0 / (base - a)
        coef[m] = a
        return a

    last = lax.fori_loop(0, n, pivot, jnp.zeros((ni, nj), jnp.float32))
    con[2] = last / (1.0 - last * last)

    @pl.loop(0, count)
    def _(s):
        rows = rows_of(s)
        r0 = PAD + pl.multiple_of(s * ROWS, ROWS)
        strong = 0.2 * mass[rows, :]
        for m in range(n):
            v = north[m, rows, :]
            low = jnp.where(lane < 1, 0.0, roll(v, 1))
            high = jnp.where(lane >= nj - 1, 0.0, roll(v, nj - 1))
            dvg[m, rows, :] = strong * (
                (up[m, pl.ds(r0 + 1, ROWS), :] - up[m, pl.ds(r0 - 1, ROWS), :]) + (high - low))

    loaded(3)
    loaded(4)

    @pl.loop(0, count)
    def _(s):
        rows = rows_of(s)
        for m in range(n):
            g = (0.5 * flip) * geo[m, rows, :]
            geo[m, rows, :] = g
            head[m, rows, :] = flip * head[m, rows, :] + g

    def lateral(it, s):
        rows = rows_of(s)
        ends = incoming(col_in[it, 0, rows, :], col_in[it, 1, rows, :])

        def level(m):
            q, end = m % per, ends[m // per]
            value = turned[m, rows, :]
            low = roll(jnp.where(couple == 2 * q, end, value), -4 * q)
            high = roll(jnp.where(couple == 2 * q + 1, end, value), -4 * q - 4)
            side[m] = low + high

        return level

    def forward(it, s):
        rows = rows_of(s)
        r0 = PAD + pl.multiple_of(s * ROWS, ROWS)
        at = pl.ds(r0, ROWS)
        weak = 0.05 * mass[rows, :]
        four = 4.0 * weak
        state = {"older": zero, "newer": None, "g": None}

        def close(m, above):
            g = head[m, rows, :] - (above - state["older"])
            if m > 0:
                g = g + coef[m - 1, rows, :] * state["g"]
            rhs[m, rows, :] = g
            state["g"] = g

        def level(m):
            ref = press[it]
            p = ref[m, at, :]
            total = (ref[m, pl.ds(r0 + 2, ROWS), :] + ref[m, pl.ds(r0 - 2, ROWS), :]) + side[m]
            d = (dvg[m, rows, :] + four * p) - weak * total
            if it < ITERS - 1:
                dvg[m, rows, :] = d
            else:
                p0[m, at, :] = (p0[m, at, :] + p1[m, at, :]) + p
            ps = p - d
            star[m, rows, :] = ps
            if m > 0:
                close(m - 1, ps)
                state["older"] = state["newer"]
            state["newer"] = ps

        def finish():
            close(n - 1, zero)
            z_out[it, 0, rows, :] = state["g"]
            z_out[it, 1, rows, :] = state["newer"]
            z_copy(it, s).start()

        return level, finish

    def col_wait(it, s):
        for t in range(2):
            col_copy(it, t, s).wait()

    def row_wait(it):
        for t in range(2):
            row_copy(it, t).wait()
        press[it][:, PAD - 2 : PAD, :] = row_in[it, 0]
        press[it][:, PAD + ni : PAD + ni + 2, :] = row_in[it, 1]

    def pass_one(it):
        col_wait(it, 1)
        level = lateral(it, 1)
        for m in range(n):
            level(m)

        @pl.loop(1, count)
        def _(s):
            @pl.when(s == count - 1)
            def _():
                row_wait(it)

            after = lax.rem(s + 1, count)
            col_wait(it, after)
            level, finish = forward(it, s)
            ahead = lateral(it, after)
            for m in range(n):
                level(m)
                ahead(m)
            finish()

        level, finish = forward(it, 0)
        for m in range(n):
            level(m)
        finish()

    def interface(it, s):
        rows = rows_of(s)
        z_copy(it, s).wait()
        a, w = coef[n - 1, rows, :], con[2, rows, :]
        mine = z_out[it, 0, rows, :] - z_in[it, 1, rows, :]
        other = z_in[it, 0, rows, :] - z_out[it, 1, rows, :]
        z = w * (mine - a * other)
        return z, a * (z - other)

    def backward(it, s):
        rows = rows_of(s)
        at = pl.ds(PAD + pl.multiple_of(s * ROWS, ROWS), ROWS)
        near, far = con[0, rows, :], con[1, rows, :]
        state = dict(zip(("z", "above"), interface(it, s)))

        def level(m):
            z = state["z"]
            g = geo[m, rows, :]
            head[m, rows, :] = near * z + g
            geo[m, rows, :] = far * z + g
            below = coef[m - 1, rows, :] * (rhs[m - 1, rows, :] + z) if m > 0 else zero
            press[it + 1][m, at, :] = star[m, rows, :] - (0.5 / STIFF) * (state["above"] - below)
            state["above"], state["z"] = z, below

        return level

    def skew(it, s):
        rows = rows_of(s)
        at = pl.ds(PAD + pl.multiple_of(s * ROWS, ROWS), ROWS)
        state = {"packs": (zero, zero)}
        quad = lane // 4

        def level(m):
            value = roll(press[it][m, at, :], 4 * (m % per) + 2)
            turned[m, rows, :] = value
            state["packs"] = placed(quad, value, m, state["packs"])

        def finish():
            outgoing(it, rows, state["packs"])
            for t in range(2):
                col_copy(it, t, s).start()

        return level, finish

    def order(t):
        return jnp.where(t < FRONT, t + 1, jnp.where(t == FRONT, count - 1, jnp.where(t == FRONT + 1, 0, t - 1)))

    def pass_two(it):
        level = backward(it, 1)
        for m in range(n - 1, -1, -1):
            level(m)

        @pl.loop(1, count)
        def _(t):
            level = backward(it, order(t))
            behind, finish = skew(it + 1, order(t - 1))
            for e in range(n):
                for m in range(2 * e, min(2 * e + 2, n)):
                    behind(n - 1 - m)
                level(n - 1 - e)
            finish()

            @pl.when(t == FRONT)
            def _():
                row_out[it + 1, 1] = press[it + 1][:, PAD + ni - 2 : PAD + ni, :]
                row_copy(it + 1, 1).start()

            @pl.when(t == FRONT + 1)
            def _():
                row_out[it + 1, 0] = press[it + 1][:, PAD : PAD + 2, :]
                row_copy(it + 1, 0).start()

        behind, finish = skew(it + 1, count - 2)
        for m in range(n - 1, -1, -1):
            behind(m)
        finish()

    for it in range(ITERS):
        pass_one(it)
        if it < ITERS - 1:
            pass_two(it)

    for t, at in ((0, PAD - 2), (1, PAD + ni)):
        p0[:, at : at + 2, :] = (row_in[0, t] + row_in[1, t]) + row_in[2, t]

    def closing(s):
        rows = rows_of(s)
        left = (col_in[0, 0, rows, :] + col_in[1, 0, rows, :]) + col_in[2, 0, rows, :]
        right = (col_in[0, 1, rows, :] + col_in[1, 1, rows, :]) + col_in[2, 1, rows, :]
        edge[0, rows, :] = jnp.where(part == 1, roll(right, -1), roll(left, 1))
        edge[1, rows, :] = jnp.where(part == 1, roll(right, 1), roll(left, -1))

    @pl.loop(0, count)
    def _(s):
        closing(s)

    @pl.loop(0, count)
    def _(t):
        s = lax.rem(t + 1, count)
        faces[0, rows_of(s), :], faces[1, rows_of(s), :] = interface(ITERS - 1, s)


def finale(n, ni, nj, rhs, star, geo, coef, psum, up, north, edge, faces, mass,
           east_out, north_out, vert_out, geo_out, press_out,
           east_s, north_s, vert_s, geo_s, press_s, sem):
    per = nj // 4
    count = ni // ROWS
    iz = lax.axis_index("gz")
    flip = (1 - 2 * iz).astype(jnp.float32)
    lane = lax.broadcasted_iota(jnp.int32, (ROWS, nj), 1)

    def store(e, src, dst, rows):
        return pltpu.make_async_copy(src.at[:, rows, :], dst.at[:, rows, :], sem.at[e])

    outs = ((east_s, east_out), (north_s, north_out), (vert_s, vert_out), (geo_s, geo_out), (press_s, press_out))

    def level_of(m):
        return iz * (n - 1) + (1 - 2 * iz) * m

    @pl.loop(0, count)
    def _(s):
        rows = pl.ds(pl.multiple_of(s * ROWS, ROWS), ROWS)
        v_of = flip / (STIFF * mass[rows, :])
        half = 0.5 * v_of
        twice = 2.0 * flip
        z, above = faces[0, rows, :], faces[1, rows, :]
        for m in range(n - 1, -1, -1):
            k = level_of(m)
            vert_s[k, rows, :] = v_of * z
            geo_s[k, rows, :] = twice * geo[m, rows, :] + half * z
            below = coef[m - 1, rows, :] * (rhs[m - 1, rows, :] + z) if m > 0 else jnp.zeros_like(z)
            press_s[k, rows, :] = star[m, rows, :] - (0.5 / STIFF) * (above - below)
            above, z = z, below
        for e in (2, 3, 4):
            store(e, *outs[e], rows).start()

    @pl.loop(0, count)
    def _(s):
        rows = pl.ds(pl.multiple_of(s * ROWS, ROWS), ROWS)
        r0 = PAD + pl.multiple_of(s * ROWS, ROWS)
        ends = (edge[0, rows, :], edge[1, rows, :])
        for m in range(n):
            k = level_of(m)
            p = psum[m, pl.ds(r0, ROWS), :]
            end = roll(ends[m // per], nj - 2 - 4 * (m % per))
            low = jnp.where(lane < 1, end, roll(p, 1))
            high = jnp.where(lane >= nj - 1, end, roll(p, nj - 1))
            north_s[k, rows, :] = north[m, rows, :] - 0.25 * (high - low)
            east_s[k, rows, :] = up[m, pl.ds(r0, ROWS), :] - 0.25 * (
                psum[m, pl.ds(r0 + 1, ROWS), :] - psum[m, pl.ds(r0 - 1, ROWS), :])
        for e in (0, 1):
            store(e, *outs[e], rows).start()

    for e in range(5):
        pltpu.make_async_copy(outs[e][0], outs[e][1], sem.at[e]).wait()


def pair(sizes, east, north, vert, geo, press, mass):
    n, ni, nj = east.shape
    f32 = jnp.float32
    count = ni // ROWS
    shape = (n, ni, nj)
    padded = (n, ni + 2 * PAD, nj)
    kept = [shape, shape, shape, shape, padded, padded, shape, (2, ni, nj), (2, ni, nj)]
    vmem = pl.BlockSpec(memory_space=pltpu.VMEM)
    state = pl.pallas_call(
        functools.partial(paired, n, ni, nj, sizes),
        out_shape=[pltpu.VMEM(s, f32) for s in kept],
        in_specs=[pl.BlockSpec(memory_space=pltpu.HBM)] * 6,
        out_specs=[vmem] * len(kept),
        scratch_shapes=[
            pltpu.VMEM(padded, f32), pltpu.VMEM(padded, f32), pltpu.VMEM(shape, f32), pltpu.VMEM(shape, f32),
            pltpu.VMEM(shape, f32),
            pltpu.VMEM((n, ROWS, nj), f32),
            pltpu.VMEM((ni, nj), f32),
            pltpu.VMEM((3, ni, nj), f32),
            pltpu.VMEM((2, ni, nj), f32),
            pltpu.VMEM((2, ni, nj), f32),
            pltpu.VMEM((ITERS, 2, n, 2, nj), f32),
            pltpu.VMEM((ITERS, 2, n, 2, nj), f32),
            pltpu.VMEM((ITERS, 2, ni, nj), f32),
            pltpu.VMEM((ITERS, 2, ni, nj), f32),
            pltpu.VMEM((ITERS, 2, ni, nj), f32),
            pltpu.VMEM((ITERS, 2, ni, nj), f32),
            pltpu.SemaphoreType.DMA((6,)),
            pltpu.SemaphoreType.DMA((ITERS, 2)),
            pltpu.SemaphoreType.DMA((ITERS, 2)),
            pltpu.SemaphoreType.DMA((ITERS, 2, count)),
            pltpu.SemaphoreType.DMA((ITERS, 2, count)),
            pltpu.SemaphoreType.DMA((ITERS, count)),
            pltpu.SemaphoreType.DMA((ITERS, count)),
        ],
        compiler_params=pltpu.CompilerParams(
            collective_id=0, has_side_effects=True, vmem_limit_bytes=41 * 1024 * 1024),
    )(east, north, vert, geo, press, mass)
    return pl.pallas_call(
        functools.partial(finale, n, ni, nj),
        out_shape=[jax.ShapeDtypeStruct(shape, f32)] * 5,
        in_specs=[vmem] * (len(kept) + 1),
        out_specs=[pl.BlockSpec(memory_space=pl.ANY)] * 5,
        scratch_shapes=[pltpu.VMEM(shape, f32)] * 5 + [pltpu.SemaphoreType.DMA((5,))],
        compiler_params=pltpu.CompilerParams(vmem_limit_bytes=18 * 1024 * 1024),
    )(*state, mass)


def solution(mesh):
    sizes = (mesh.shape["gx"], mesh.shape["gy"], mesh.shape["gz"])
    cube = P("gz", "gx", "gy")

    def body(east, *rest):
        n, ni, nj = east.shape
        fits = sizes[2] == 2 and n <= nj // 2 and ni // ROWS > FRONT + 2 and ni % WIDE == 0 and ITERS == 3
        return (pair if fits else local)(sizes, east, *rest)

    return jax.shard_map(
        body, mesh=mesh,
        in_specs=(cube,) * 5 + (P("gx", "gy"),), out_specs=(cube,) * 5, check_vma=False)
```

```python
import functools

import jax
import jax.numpy as jnp
from jax import lax
from jax.experimental import pallas as pl
from jax.experimental.pallas import tpu as pltpu
from jax.sharding import PartitionSpec as P

ITERS = 3
STIFF = 30.0
PAD = 8
ROWS = 16
PARTS = 2
UNROLL = 24


def roll(value, shift):
    if isinstance(shift, int):
        shift = shift % value.shape[1]
    return pltpu.roll(value, shift, 1)


def kernel(n, ni, nj, sizes, east_in, north_in, vert_in, geo_in, press_in, mass,
           east, north, vert, geo, press,
           pp, up, psum, dvg, mu_s, c_s, planes, bounds,
           row_out, row_in, col_out, col_in, z_out, z_in,
           load_sem, row_send, row_recv, col_send, col_recv, z_send, z_recv):
    nx, ny, nz = sizes
    unroll = max(u for u in range(2, UNROLL + 1) if n % u == 0 and u % 2 == 0)
    ix, iy, iz = lax.axis_index("gx"), lax.axis_index("gy"), lax.axis_index("gz")
    xs = (lax.rem(ix + nx - 1, nx), lax.rem(ix + 1, nx))
    ys = (lax.rem(iy + ny - 1, ny), lax.rem(iy + 1, ny))

    loads = [
        pltpu.make_async_copy(press_in, pp.at[:, pl.ds(PAD, ni), :], load_sem.at[0]),
        pltpu.make_async_copy(east_in, up.at[:, pl.ds(PAD, ni), :], load_sem.at[1]),
        pltpu.make_async_copy(north_in, north, load_sem.at[2]),
        pltpu.make_async_copy(vert_in, vert, load_sem.at[3]),
        pltpu.make_async_copy(geo_in, geo, load_sem.at[4]),
    ]
    for load in loads:
        load.start()

    barrier = pltpu.get_barrier_semaphore()
    for t in range(2):
        pl.semaphore_signal(barrier, inc=1, device_id={"gx": xs[t]})
        pl.semaphore_signal(barrier, inc=1, device_id={"gy": ys[t]})
    for d in range(1, nz):
        pl.semaphore_signal(barrier, inc=1, device_id={"gz": lax.rem(iz + d, nz)})
    pl.semaphore_wait(barrier, 4 + nz - 1)

    def row_copy(slot, t):
        return pltpu.make_async_remote_copy(
            src_ref=row_out.at[slot, t], dst_ref=row_in.at[slot, 1 - t],
            send_sem=row_send.at[slot, t], recv_sem=row_recv.at[slot, 1 - t],
            device_id={"gx": xs[t]})

    span = ni // PARTS

    def part_rows(h):
        return pl.ds(pl.multiple_of(h * span, span), span)

    def col_copy(slot, t, h):
        return pltpu.make_async_remote_copy(
            src_ref=col_out.at[slot, t, part_rows(h), :], dst_ref=col_in.at[slot, 1 - t, part_rows(h), :],
            send_sem=col_send.at[slot, t, h], recv_sem=col_recv.at[slot, 1 - t, h],
            device_id={"gy": ys[t]})

    def z_copy(slot, d, h):
        return pltpu.make_async_remote_copy(
            src_ref=z_out.at[slot, :, part_rows(h), :], dst_ref=z_in.at[slot, d - 1, :, part_rows(h), :],
            send_sem=z_send.at[slot, d - 1, h], recv_sem=z_recv.at[slot, d - 1, h],
            device_id={"gz": lax.rem(iz + d, nz)})

    lane = lax.broadcasted_iota(jnp.int32, (ROWS, nj), 1)
    pair = lane // 2

    def merged(left, right, width):
        left, right = roll(left, width), roll(right, nj - width)
        even = pair % 2 == 0
        return jnp.where(even, right, left), jnp.where(even, left, right)

    def send_rows(slot, ref):
        row_out[slot, 0] = ref[:, PAD : PAD + 2, :]
        row_out[slot, 1] = ref[:, PAD + ni - 2 : PAD + ni, :]
        for t in range(2):
            row_copy(slot, t).start()

    def recv_rows(slot, ref):
        for t in range(2):
            row_copy(slot, t).wait()
        ref[:, PAD - 2 : PAD, :] = row_in[slot, 0]
        ref[:, PAD + ni : PAD + ni + 2, :] = row_in[slot, 1]

    def packed(value, k, packs):
        turned = roll(value, 2 * k + 2)
        return (jnp.where(pair == k + 1, turned, packs[0]), jnp.where(pair == k, turned, packs[1]))

    def strips(body, h=None):
        count = (ni if h is None else span) // ROWS
        first = 0 if h is None else h * count

        @pl.loop(0, count)
        def _(s):
            body(pl.multiple_of((first + s) * ROWS, ROWS))

    def send_cols(slot, load_level):
        def body(r0):
            zero = jnp.zeros((ROWS, nj), jnp.float32)

            def group(q, packs):
                for e in range(unroll):
                    k = q * unroll + e
                    packs = packed(load_level(k, r0), k, packs)
                return packs

            packs = lax.fori_loop(0, n // unroll, group, (zero, zero))
            for t in range(2):
                col_out[slot, t, pl.ds(r0, ROWS), :] = packs[t]

        strips(body)
        for h in range(PARTS):
            for t in range(2):
                col_copy(slot, t, h).start()

    loads[0].wait()
    send_rows(0, pp)
    send_cols(0, lambda k, r0: pp[k, pl.ds(PAD + r0, ROWS), :])
    loads[1].wait()
    send_rows(ITERS, up)
    loads[2].wait()
    send_cols(ITERS, lambda k, r0: north[k, pl.ds(r0, ROWS), :])

    stiff = STIFF * mass[...]
    root = jnp.sqrt(1.0 + 4.0 * stiff)
    major = 0.5 * (1.0 + 2.0 * stiff + root)
    mu_s[...] = stiff / major
    c_s[...] = 1.0 / major
    planes[0] = jnp.log(stiff / major)
    planes[1] = major / root
    planes[2] = major / stiff

    recv_rows(0, pp)
    recv_rows(ITERS, up)
    for slot in (0, ITERS):
        for t in range(2):
            for h in range(PARTS):
                col_copy(slot, t, h).wait()
    loads[3].wait()
    loads[4].wait()

    def pass_one(it, h):
        def body(r0):
            rows = pl.ds(r0, ROWS)
            m, mu, c = mass[rows, :], mu_s[rows, :], c_s[rows, :]
            weak, strong = 0.05 * m, 0.2 * m
            left, right = col_in[it, 0, rows, :], col_in[it, 1, rows, :]
            ends = merged(left, right, 2)
            if it == 0:
                vends = merged(col_in[ITERS, 0, rows, :], col_in[ITERS, 1, rows, :], 1)

            def star(k, parity):
                end = roll(ends[parity], nj - 2 - 2 * k)
                at = pl.ds(PAD + r0, ROWS)
                p = pp[k, at, :]
                low = jnp.where(lane < 2, end, roll(p, 2))
                high = jnp.where(lane >= nj - 2, end, roll(p, nj - 2))
                total = (pp[k, pl.ds(PAD + r0 + 2, ROWS), :] + pp[k, pl.ds(PAD + r0 - 2, ROWS), :]) + (low + high) - 4.0 * p
                if it == 0:
                    v = north[k, rows, :]
                    vend = roll(vends[parity], nj - 2 - 2 * k)
                    vlow = jnp.where(lane < 1, vend, roll(v, 1))
                    vhigh = jnp.where(lane >= nj - 1, vend, roll(v, nj - 1))
                    d = strong * (up[k, pl.ds(PAD + r0 + 1, ROWS), :] - up[k, pl.ds(PAD + r0 - 1, ROWS), :] + (vhigh - vlow))
                    psum[k, at, :] = p
                else:
                    d = dvg[k, rows, :]
                    psum[k, at, :] = psum[k, at, :] + p
                d = d - weak * total
                if it < ITERS - 1:
                    dvg[k, rows, :] = d
                ps = p - d
                press[k, rows, :] = ps
                return ps

            def sweep(k, above, below, state):
                y, dn, weight = state
                f = c * (vert[k, rows, :] + 0.5 * geo[k, rows, :] - (above - below))
                y = mu * y + f
                vert[k, rows, :] = y
                return y, dn + weight * f, weight * mu

            def steps(ks, carry):
                older, newer, state = carry
                for e, k in enumerate(ks):
                    ps = star(k, e % 2)
                    if not (isinstance(k, int) and k == 0):
                        state = sweep(k - 1, ps, older, state)
                    older, newer = newer, ps
                return older, newer, state

            zero = jnp.zeros((ROWS, nj), jnp.float32)
            carry = (zero, zero, (zero, zero, zero + 1.0))
            carry = steps(range(unroll), carry)
            planes_lo = press[0, rows, :]

            def group(q, carry):
                return steps([q * unroll + e for e in range(unroll)], carry)

            older, newer, state = lax.fori_loop(1, n // unroll, group, carry)
            y, dn, _ = sweep(n - 1, zero, older, state)
            z_out[it, 0, rows, :] = y
            z_out[it, 1, rows, :] = dn
            z_out[it, 2, rows, :] = c * planes_lo
            z_out[it, 3, rows, :] = c * newer

        strips(body, h)

    def interface(it, h):
        def body(r0):
            rows = pl.ds(r0, ROWS)
            mu, logmu, kappa, inv = mu_s[rows, :], planes[0, rows, :], planes[1, rows, :], planes[2, rows, :]
            zero = jnp.zeros((ROWS, nj), jnp.float32)

            def power(m):
                if not isinstance(m, int):
                    m = jnp.maximum(m, 0).astype(jnp.float32)
                return jnp.exp(m * logmu)

            near = power(n - 1)
            below, above, to_low, to_high = zero, zero, zero, zero
            pieces = {}

            def piece(d, which):
                if abs(d) >= nz:
                    return zero
                if d == 0:
                    return z_out[it, which, rows, :]
                value = z_in[it, (nz - d - 1) % nz if d > 0 else -d - 1, which, rows, :]
                inside = jnp.logical_and(iz + d >= 0, iz + d < nz)
                return jnp.where(inside, value, 0.0)

            own_up = own_dn = zero
            for d in range(-(nz - 1), nz):
                j = iz + d
                inside = jnp.logical_and(j >= 0, j < nz)
                under, over = piece(d - 1, 3), piece(d + 1, 2)
                upt = piece(d, 0) + near * under - over
                dnt = piece(d, 1) + under - near * over
                if d == 0:
                    own_up, own_dn = upt, dnt
                    delta_low, delta_high = under, over
                elif d < 0:
                    below = below + jnp.where(inside, power(n * (-1 - d)) * upt, 0.0)
                else:
                    above = above + jnp.where(inside, power(n * (d - 1)) * dnt, 0.0)
                to_low = to_low + jnp.where(inside, power(n * j + 1) * dnt, 0.0)
                to_high = to_high + jnp.where(inside, power(n * (nz - 1 - j) + 1) * upt, 0.0)
            q = power(n * nz + 1)
            scale = kappa / (1.0 - q * q)
            alpha = kappa * below + (q * to_high - to_low) * scale * power(n * iz)
            beta = kappa * above + (q * to_low - to_high) * scale * power(n * (nz - 1 - iz))
            far = power(n + 1)
            bounds[2, rows, :] = kappa * mu * own_dn + alpha + beta * far
            bounds[3, rows, :] = kappa * mu * own_up + beta + alpha * far
            alpha = alpha + kappa * delta_low * inv
            beta = beta - kappa * delta_high * inv
            bounds[0, rows, :] = kappa * mu * z_out[it, 0, rows, :] + beta
            bounds[1, rows, :] = alpha * power(n)

        strips(body, h)

    def pass_two(it, h):
        last = it == ITERS - 1

        def body(r0):
            rows = pl.ds(r0, ROWS)
            mu, inv = mu_s[rows, :], planes[2, rows, :]
            half = 0.5 * mass[rows, :]
            zero = jnp.zeros((ROWS, nj), jnp.float32)

            def finish(k, above, below, packs):
                p = press[k, rows, :] - half * (above - below)
                if last:
                    press[k, rows, :] = p
                    return packs
                pp[k, pl.ds(PAD + r0, ROWS), :] = p
                return packed(p, k, packs)

            def steps(ks, carry):
                x, h, older, newer, packs = carry
                for k in ks:
                    x = mu * x + vert[k, rows, :]
                    v = x + h
                    h = h * inv
                    vert[k, rows, :] = v
                    geo[k, rows, :] = geo[k, rows, :] + 0.5 * v
                    if not (isinstance(k, int) and k == n - 1):
                        packs = finish(k + 1, older, v, packs)
                    older, newer = newer, v
                return x, h, older, newer, packs

            top = bounds[3, rows, :]
            carry = (bounds[0, rows, :], bounds[1, rows, :], zero, top, (zero, zero))
            carry = steps([n - 1 - e for e in range(unroll)], carry)

            def group(q, carry):
                return steps([n - 1 - q * unroll - e for e in range(unroll)], carry)

            _, _, older, newer, packs = lax.fori_loop(1, n // unroll, group, carry)
            packs = finish(0, older, bounds[2, rows, :], packs)
            if not last:
                for t in range(2):
                    col_out[it + 1, t, rows, :] = packs[t]

        strips(body, h)

    def winds():
        def body(r0):
            rows = pl.ds(r0, ROWS)
            left = col_in[0, 0, rows, :]
            right = col_in[0, 1, rows, :]
            for it in range(1, ITERS):
                left = left + col_in[it, 0, rows, :]
                right = right + col_in[it, 1, rows, :]

            ends = merged(left, right, 1)

            def group(q, carry):
                for e in range(unroll):
                    k = q * unroll + e
                    end = roll(ends[e % 2], nj - 2 - 2 * k)
                    at = pl.ds(PAD + r0, ROWS)
                    p = psum[k, at, :]
                    east[k, rows, :] = up[k, at, :] - 0.25 * (
                        psum[k, pl.ds(PAD + r0 + 1, ROWS), :] - psum[k, pl.ds(PAD + r0 - 1, ROWS), :])
                    low = jnp.where(lane < 1, end, roll(p, 1))
                    high = jnp.where(lane >= nj - 1, end, roll(p, nj - 1))
                    north[k, rows, :] = north[k, rows, :] - 0.25 * (high - low)
                return carry

            lax.fori_loop(0, n // unroll, group, 0)

        strips(body)

    for it in range(ITERS):
        if it > 0:
            recv_rows(it, pp)

        @pl.loop(0, PARTS)
        def _(h, it=it):
            if it > 0:
                for t in range(2):
                    col_copy(it, t, h).wait()
            pass_one(it, h)
            for d in range(1, nz):
                z_copy(it, d, h).start()

        if it == ITERS - 1:
            for t, at in ((0, PAD - 2), (1, PAD + ni)):
                total = row_in[0, t]
                for slot in range(1, ITERS):
                    total = total + row_in[slot, t]
                psum[:, at : at + 2, :] = total
            winds()

        @pl.loop(0, PARTS)
        def _(h, it=it):
            for d in range(1, nz):
                z_copy(it, d, h).wait()
            interface(it, h)
            pass_two(it, h)
            if it < ITERS - 1:
                for t in range(2):
                    col_copy(it + 1, t, h).start()

        if it < ITERS - 1:
            send_rows(it + 1, pp)


def local(sizes, east, north, vert, geo, press, mass):
    n, ni, nj = east.shape
    nz = sizes[2]
    f32 = jnp.float32
    slots = ITERS + 1
    field = pltpu.VMEM((n, ni, nj), f32)
    padded = pltpu.VMEM((n, ni + 2 * PAD, nj), f32)
    plane = pltpu.VMEM((ni, nj), f32)
    return pl.pallas_call(
        functools.partial(kernel, n, ni, nj, sizes),
        out_shape=[pltpu.VMEM((n, ni, nj), f32)] * 5,
        in_specs=[pl.BlockSpec(memory_space=pl.ANY)] * 5 + [pl.BlockSpec(memory_space=pltpu.VMEM)],
        out_specs=[pl.BlockSpec(memory_space=pltpu.VMEM)] * 5,
        scratch_shapes=[
            padded, padded, padded, field, plane, plane,
            pltpu.VMEM((3, ni, nj), f32),
            pltpu.VMEM((4, ni, nj), f32),
            pltpu.VMEM((slots, 2, n, 2, nj), f32),
            pltpu.VMEM((slots, 2, n, 2, nj), f32),
            pltpu.VMEM((slots, 2, ni, nj), f32),
            pltpu.VMEM((slots, 2, ni, nj), f32),
            pltpu.VMEM((ITERS, 4, ni, nj), f32),
            pltpu.VMEM((ITERS, nz - 1, 4, ni, nj), f32),
            pltpu.SemaphoreType.DMA((5,)),
            pltpu.SemaphoreType.DMA((slots, 2)),
            pltpu.SemaphoreType.DMA((slots, 2)),
            pltpu.SemaphoreType.DMA((slots, 2, PARTS)),
            pltpu.SemaphoreType.DMA((slots, 2, PARTS)),
            pltpu.SemaphoreType.DMA((ITERS, nz - 1, PARTS)),
            pltpu.SemaphoreType.DMA((ITERS, nz - 1, PARTS)),
        ],
        compiler_params=pltpu.CompilerParams(
            collective_id=0, has_side_effects=True, vmem_limit_bytes=40 * 1024 * 1024),
    )(east, north, vert, geo, press, mass)


LAG = 3
TILE = 32
WIDE = 32


def paired(n, ni, nj, sizes, east_in, north_in, vert_in, geo_in, press_in, mass_in,
           rhs, star, geo, coef, p0, up, north, edge, faces,
           p1, p2, dvg, head, turned_a, turned_b, turned_c, side, mass, con, packs_p, packs_v,
           row_out, row_in, col_out, col_in, z_out, z_in,
           load_sem, row_send, row_recv, col_send, col_recv, z_send, z_recv):
    nx, ny, _ = sizes
    per = nj // 4
    count = ni // TILE
    press = (p0, p1, p2)
    turned = (turned_a, turned_c, turned_a)
    ix, iy, iz = lax.axis_index("gx"), lax.axis_index("gy"), lax.axis_index("gz")
    xs = (lax.rem(ix + nx - 1, nx), lax.rem(ix + 1, nx))
    ys = (lax.rem(iy + ny - 1, ny), lax.rem(iy + 1, ny))
    flip = (1 - 2 * iz).astype(jnp.float32)
    half = 0.5 * flip
    inner = pl.ds(PAD, ni)

    barrier = pltpu.get_barrier_semaphore()
    for t in range(2):
        pl.semaphore_signal(barrier, inc=1, device_id={"gx": xs[t]})
        pl.semaphore_signal(barrier, inc=1, device_id={"gy": ys[t]})
    pl.semaphore_signal(barrier, inc=1, device_id={"gz": 1 - iz})

    mass_load = pltpu.make_async_copy(mass_in, mass, load_sem.at[5])
    mass_load.start()
    fields = (
        (press_in, p0.at[:, inner, :]), (north_in, north), (east_in, up.at[:, inner, :]),
        (vert_in, head), (geo_in, geo))

    def load(e, m):
        src, dst = fields[e]
        k = iz * (n - 1) + (1 - 2 * iz) * m
        pltpu.make_async_copy(src.at[k], dst.at[m], load_sem.at[e]).start()

    def loaded(e):
        pltpu.make_async_copy(fields[e][0], fields[e][1], load_sem.at[e]).wait()

    @pl.loop(0, n)
    def _(m):
        load(0, m)

    def row_copy(it, t):
        return pltpu.make_async_remote_copy(
            src_ref=row_out.at[it, t], dst_ref=row_in.at[it, 1 - t],
            send_sem=row_send.at[it, t], recv_sem=row_recv.at[it, 1 - t],
            device_id={"gx": xs[t]})

    def rows_of(s):
        return pl.ds(pl.multiple_of(s * TILE, TILE), TILE)

    def col_copy(it, t, s):
        return pltpu.make_async_remote_copy(
            src_ref=col_out.at[it, t, rows_of(s), :], dst_ref=col_in.at[it, 1 - t, rows_of(s), :],
            send_sem=col_send.at[it, t, s], recv_sem=col_recv.at[it, 1 - t, s],
            device_id={"gy": ys[t]})

    def z_copy(it, s):
        return pltpu.make_async_remote_copy(
            src_ref=z_out.at[it, :, rows_of(s), :], dst_ref=z_in.at[it, :, rows_of(s), :],
            send_sem=z_send.at[it, s], recv_sem=z_recv.at[it, s],
            device_id={"gz": 1 - iz})

    lane = lax.broadcasted_iota(jnp.int32, (TILE, nj), 1)
    part, couple, quad = lane % 4, lane // 2, lane // 4
    zero = jnp.zeros((TILE, nj), jnp.float32)
    whole = lax.broadcasted_iota(jnp.int32, (ni, nj), 1) % 4

    def placed(mask, value, m, packs):
        b = m // per
        return tuple(jnp.where(mask, value, packs[c]) if c == b else packs[c] for c in range(2))

    def outgoing(it, rows, part, packs):
        a, b = packs
        col_out[it, 0, rows, :] = jnp.where(part >= 2, a, roll(b, -2))
        col_out[it, 1, rows, :] = jnp.where(part < 2, a, roll(b, 2))

    mass_load.wait()
    inverse = 1.0 / (STIFF * mass[...])
    con[0] = 1.25 * inverse
    con[1] = 0.25 * inverse
    base = 2.0 + inverse

    def pivot(m, a):
        load(1, m)
        a = 1.0 / (base - a)
        coef[m] = a
        return a

    last = lax.fori_loop(0, n, pivot, jnp.zeros((ni, nj), jnp.float32))
    con[2] = last / (1.0 - last * last)

    wide = lax.broadcasted_iota(jnp.int32, (WIDE, nj), 1)
    blank = jnp.zeros((WIDE, nj), jnp.float32)
    share = n * WIDE // ni

    loaded(0)

    @pl.loop(0, ni // WIDE)
    def _(b):
        r0 = pl.multiple_of(b * WIDE, WIDE)
        rows = pl.ds(r0, WIDE)
        packs = (blank, blank)
        for m in range(n):
            value = roll(p0[m, pl.ds(PAD + r0, WIDE), :], 4 * (m % per) + 2)
            turned_a[m, rows, :] = value
            packs = placed(wide // 4 == m % per, value, m, packs)
            if m < share:
                load(2, b * share + m)
        packs_p[0, rows, :], packs_p[1, rows, :] = packs

    loaded(1)

    @pl.loop(0, ni // WIDE)
    def _(b):
        r0 = pl.multiple_of(b * WIDE, WIDE)
        rows = pl.ds(r0, WIDE)
        packs = (blank, blank)
        for m in range(n):
            q = 4 * (m % per)
            value = roll(4.0 * north[m, rows, :], q + 1)
            turned_b[m, rows, :] = turned_a[m, rows, :] + value
            packs = placed(wide // 2 == q // 2, value, m, packs)
            if m < share:
                load(3, b * share + m)
                load(4, b * share + m)
        packs_v[0, rows, :], packs_v[1, rows, :] = packs

    edges = []
    for c in range(2):
        v = packs_v[c]
        back = roll(v, 2)
        edges.append(packs_p[c] + jnp.where(whole == 0, v, jnp.where(whole == 3, -back, 0.0)))
        packs_v[c] = jnp.where(whole == 1, v, jnp.where(whole == 2, -back, 0.0))
    outgoing(0, slice(None), whole, edges)

    pl.semaphore_wait(barrier, 5)

    @pl.loop(0, count)
    def _(t):
        s = lax.rem(t + 1, count)
        for t in range(2):
            col_copy(0, t, s).start()

    loaded(2)
    up[:, :PAD, :] = jnp.zeros((n, PAD, nj), jnp.float32)
    up[:, PAD + ni :, :] = jnp.zeros((n, PAD, nj), jnp.float32)
    row_out[0, 0] = p0[:, PAD : PAD + 2, :] - 4.0 * up[:, PAD - 1 : PAD + 1, :]
    row_out[0, 1] = p0[:, PAD + ni - 2 : PAD + ni, :] + 4.0 * up[:, PAD + ni - 1 : PAD + ni + 1, :]
    for t in range(2):
        row_copy(0, t).start()

    @pl.loop(0, ni // WIDE)
    def _(b):
        rows = pl.ds(pl.multiple_of(b * WIDE, WIDE), WIDE)
        for m in range(n):
            turned_a[m, rows, :] = turned_a[m, rows, :] - roll(4.0 * north[m, rows, :], 4 * (m % per) + 3)

    loaded(3)
    loaded(4)

    def lateral(it, s):
        rows = rows_of(s)
        left, right = col_in[it, 0, rows, :], col_in[it, 1, rows, :]
        ends = (jnp.where(part < 2, left, right), jnp.where(part < 2, roll(left, -2), roll(right, 2)))
        if it == 0:
            ends = [ends[c] + packs_v[c, rows, :] for c in range(2)]

        def level(m):
            q, end = m % per, ends[m // per]
            lower = upper = turned[it][m, rows, :]
            if it == 0:
                lower = turned_b[m, rows, :]
            low = roll(jnp.where(couple == 2 * q, end, lower), -4 * q)
            high = roll(jnp.where(couple == 2 * q + 1, end, upper), -4 * q - 4)
            side[m] = low + high

        return level

    def forward(it, s):
        rows = rows_of(s)
        r0 = PAD + pl.multiple_of(s * TILE, TILE)
        at = pl.ds(r0, TILE)
        weak = 0.05 * mass[rows, :]
        four = 4.0 * weak
        state = {"older": zero, "newer": None, "g": None}

        def close(m, above):
            own = head[m, rows, :]
            if it == 0:
                own = flip * own + half * geo[m, rows, :]
            g = own - (above - state["older"])
            if m > 0:
                g = g + coef[m - 1, rows, :] * state["g"]
            rhs[m, rows, :] = g
            state["g"] = g

        def level(m):
            ref = press[it]
            p = ref[m, at, :]
            total = (ref[m, pl.ds(r0 + 2, TILE), :] + ref[m, pl.ds(r0 - 2, TILE), :]) + side[m]
            d = four * p
            if it == 0:
                total = total - 4.0 * (up[m, pl.ds(r0 + 1, TILE), :] - up[m, pl.ds(r0 - 1, TILE), :])
            else:
                d = dvg[m, rows, :] + d
            d = d - weak * total
            if it < ITERS - 1:
                dvg[m, rows, :] = d
            else:
                p0[m, at, :] = (p0[m, at, :] + p1[m, at, :]) + p
            ps = p - d
            star[m, rows, :] = ps
            if m > 0:
                close(m - 1, ps)
                state["older"] = state["newer"]
            state["newer"] = ps

        def finish():
            close(n - 1, zero)
            z_out[it, 0, rows, :] = state["g"]
            z_out[it, 1, rows, :] = state["newer"]
            z_copy(it, s).start()

        return level, finish

    def col_wait(it, s):
        for t in range(2):
            col_copy(it, t, s).wait()

    def row_wait(it):
        for t in range(2):
            row_copy(it, t).wait()
        press[it][:, PAD - 2 : PAD, :] = row_in[it, 0]
        press[it][:, PAD + ni : PAD + ni + 2, :] = row_in[it, 1]

    def meet(a, w, out, inn):
        mine, other = out[0] - inn[1], inn[0] - out[1]
        z = w * (mine - a * other)
        return z, a * (z - other)

    def backward(it, s):
        rows = rows_of(s)
        at = pl.ds(PAD + pl.multiple_of(s * TILE, TILE), TILE)
        near, far = con[0, rows, :], con[1, rows, :]
        z_copy(it, s).wait()
        state = {"packs": (zero, zero)}
        state["z"], state["above"] = meet(
            coef[n - 1, rows, :], con[2, rows, :],
            [z_out[it, c, rows, :] for c in range(2)], [z_in[it, c, rows, :] for c in range(2)])

        def level(m):
            z = state["z"]
            g = geo[m, rows, :]
            if it == 0:
                g = half * g
            head[m, rows, :] = near * z + g
            geo[m, rows, :] = far * z + g
            below = coef[m - 1, rows, :] * (rhs[m - 1, rows, :] + z) if m > 0 else zero
            p = star[m, rows, :] - (0.5 / STIFF) * (state["above"] - below)
            press[it + 1][m, at, :] = p
            value = roll(p, 4 * (m % per) + 2)
            turned[it + 1][m, rows, :] = value
            state["packs"] = placed(quad == m % per, value, m, state["packs"])
            state["above"], state["z"] = z, below

        def finish():
            outgoing(it + 1, rows, part, state["packs"])
            for t in range(2):
                col_copy(it + 1, t, s).start()

        return level, finish

    for it in range(ITERS):
        final = it == ITERS - 1
        front = (count - 2, count - 2, count - 2)[it]
        lag = count if final else LAG

        def order(t, front=front):
            return jnp.where(t < front, t + 1, jnp.where(t == front, count - 1, jnp.where(t == front + 1, 0, t - 1)))

        def ahead_of(t, it=it, front=front, order=order):
            @pl.when(t == front)
            def _():
                row_wait(it)

            after = order(lax.rem(t + 1, count))

            @pl.when(t < count - 1)
            def _():
                col_wait(it, after)

            return forward(it, order(t)) + (lateral(it, after),)

        def behind(u, it=it, order=order):
            return backward(it, order(u))

        def send_rows(u, it=it, front=front):
            @pl.when(u == front)
            def _():
                row_out[it + 1, 1] = press[it + 1][:, PAD + ni - 2 : PAD + ni, :]
                row_copy(it + 1, 1).start()

            @pl.when(u == front + 1)
            def _():
                row_out[it + 1, 0] = press[it + 1][:, PAD : PAD + 2, :]
                row_copy(it + 1, 0).start()

        col_wait(it, order(0))
        first = lateral(it, order(0))
        for m in range(n):
            first(m)

        @pl.loop(0, lag)
        def _(t):
            one, finish, ahead = ahead_of(t)
            for m in range(n):
                one(m)
                ahead(m)
            finish()

        if not final:
            @pl.loop(lag, count)
            def _(t):
                one, finish, ahead = ahead_of(t)
                for m in range(n):
                    one(m)
                    ahead(m)
                finish()
                two, deliver = behind(t - lag)
                for m in range(n):
                    two(n - 1 - m)
                deliver()
                send_rows(t - lag)

            @pl.loop(count - lag, count)
            def _(u):
                two, deliver = behind(u)
                for m in range(n):
                    two(n - 1 - m)
                deliver()
                send_rows(u)

    for t, at in ((0, PAD - 2), (1, PAD + ni)):
        p0[:, at : at + 2, :] = (row_in[0, t] + row_in[1, t]) + row_in[2, t]
    left = (col_in[0, 0] + col_in[1, 0]) + col_in[2, 0]
    right = (col_in[0, 1] + col_in[1, 1]) + col_in[2, 1]
    edge[0] = jnp.where(whole == 1, roll(right, -1), roll(left, 1))
    edge[1] = jnp.where(whole == 1, roll(right, 1), roll(left, -1))

    @pl.loop(0, count)
    def _(s):
        z_copy(ITERS - 1, s).wait()

    faces[0], faces[1] = meet(
        coef[n - 1], con[2], [z_out[ITERS - 1, c] for c in range(2)], [z_in[ITERS - 1, c] for c in range(2)])


def finale(n, ni, nj, rhs, star, geo, coef, psum, up, north, edge, faces, mass,
           east_out, north_out, vert_out, geo_out, press_out,
           east_s, north_s, vert_s, geo_s, press_s, sem):
    per = nj // 4
    count = ni // ROWS
    iz = lax.axis_index("gz")
    flip = (1 - 2 * iz).astype(jnp.float32)
    lane = lax.broadcasted_iota(jnp.int32, (ROWS, nj), 1)

    def store(e, src, dst, rows):
        return pltpu.make_async_copy(src.at[:, rows, :], dst.at[:, rows, :], sem.at[e])

    outs = ((east_s, east_out), (north_s, north_out), (vert_s, vert_out), (geo_s, geo_out), (press_s, press_out))

    def level_of(m):
        return iz * (n - 1) + (1 - 2 * iz) * m

    @pl.loop(0, count)
    def _(s):
        rows = pl.ds(pl.multiple_of(s * ROWS, ROWS), ROWS)
        v_of = flip / (STIFF * mass[rows, :])
        half = 0.5 * v_of
        twice = 2.0 * flip
        z, above = faces[0, rows, :], faces[1, rows, :]
        for m in range(n - 1, -1, -1):
            k = level_of(m)
            vert_s[k, rows, :] = v_of * z
            geo_s[k, rows, :] = twice * geo[m, rows, :] + half * z
            below = coef[m - 1, rows, :] * (rhs[m - 1, rows, :] + z) if m > 0 else jnp.zeros_like(z)
            press_s[k, rows, :] = star[m, rows, :] - (0.5 / STIFF) * (above - below)
            above, z = z, below
        for e in (2, 3, 4):
            store(e, *outs[e], rows).start()

    @pl.loop(0, count)
    def _(s):
        rows = pl.ds(pl.multiple_of(s * ROWS, ROWS), ROWS)
        r0 = PAD + pl.multiple_of(s * ROWS, ROWS)
        ends = (edge[0, rows, :], edge[1, rows, :])
        for m in range(n):
            k = level_of(m)
            p = psum[m, pl.ds(r0, ROWS), :]
            end = roll(ends[m // per], nj - 2 - 4 * (m % per))
            low = jnp.where(lane < 1, end, roll(p, 1))
            high = jnp.where(lane >= nj - 1, end, roll(p, nj - 1))
            north_s[k, rows, :] = north[m, rows, :] - 0.25 * (high - low)
            east_s[k, rows, :] = up[m, pl.ds(r0, ROWS), :] - 0.25 * (
                psum[m, pl.ds(r0 + 1, ROWS), :] - psum[m, pl.ds(r0 - 1, ROWS), :])
        for e in (0, 1):
            store(e, *outs[e], rows).start()

    for e in range(5):
        pltpu.make_async_copy(outs[e][0], outs[e][1], sem.at[e]).wait()


def pair(sizes, east, north, vert, geo, press, mass):
    n, ni, nj = east.shape
    f32 = jnp.float32
    count = ni // TILE
    shape = (n, ni, nj)
    padded = (n, ni + 2 * PAD, nj)
    kept = [shape, shape, shape, shape, padded, padded, shape, (2, ni, nj), (2, ni, nj)]
    vmem = pl.BlockSpec(memory_space=pltpu.VMEM)
    state = pl.pallas_call(
        functools.partial(paired, n, ni, nj, sizes),
        out_shape=[pltpu.VMEM(s, f32) for s in kept],
        in_specs=[pl.BlockSpec(memory_space=pltpu.HBM)] * 6,
        out_specs=[vmem] * len(kept),
        scratch_shapes=[
            pltpu.VMEM(padded, f32), pltpu.VMEM(padded, f32), pltpu.VMEM(shape, f32), pltpu.VMEM(shape, f32),
            pltpu.VMEM(shape, f32), pltpu.VMEM(shape, f32), pltpu.VMEM(shape, f32),
            pltpu.VMEM((n, TILE, nj), f32),
            pltpu.VMEM((ni, nj), f32),
            pltpu.VMEM((3, ni, nj), f32),
            pltpu.VMEM((2, ni, nj), f32),
            pltpu.VMEM((2, ni, nj), f32),
            pltpu.VMEM((ITERS, 2, n, 2, nj), f32),
            pltpu.VMEM((ITERS, 2, n, 2, nj), f32),
            pltpu.VMEM((ITERS, 2, ni, nj), f32),
            pltpu.VMEM((ITERS, 2, ni, nj), f32),
            pltpu.VMEM((ITERS, 2, ni, nj), f32),
            pltpu.VMEM((ITERS, 2, ni, nj), f32),
            pltpu.SemaphoreType.DMA((6,)),
            pltpu.SemaphoreType.DMA((ITERS, 2)),
            pltpu.SemaphoreType.DMA((ITERS, 2)),
            pltpu.SemaphoreType.DMA((ITERS, 2, count)),
            pltpu.SemaphoreType.DMA((ITERS, 2, count)),
            pltpu.SemaphoreType.DMA((ITERS, count)),
            pltpu.SemaphoreType.DMA((ITERS, count)),
        ],
        compiler_params=pltpu.CompilerParams(
            collective_id=0, has_side_effects=True, vmem_limit_bytes=41 * 1024 * 1024),
    )(east, north, vert, geo, press, mass)
    return pl.pallas_call(
        functools.partial(finale, n, ni, nj),
        out_shape=[jax.ShapeDtypeStruct(shape, f32)] * 5,
        in_specs=[vmem] * (len(kept) + 1),
        out_specs=[pl.BlockSpec(memory_space=pl.ANY)] * 5,
        scratch_shapes=[pltpu.VMEM(shape, f32)] * 5 + [pltpu.SemaphoreType.DMA((5,))],
        compiler_params=pltpu.CompilerParams(vmem_limit_bytes=18 * 1024 * 1024),
    )(*state, mass)


def solution(mesh):
    sizes = (mesh.shape["gx"], mesh.shape["gy"], mesh.shape["gz"])
    cube = P("gz", "gx", "gy")

    def body(east, *rest):
        n, ni, nj = east.shape
        fits = sizes[2] == 2 and n <= nj // 2 and ni % TILE == 0 and ni // TILE > LAG and ni % WIDE == 0 and n * WIDE % ni == 0 and ITERS == 3
        return (pair if fits else local)(sizes, east, *rest)

    return jax.shard_map(
        body, mesh=mesh,
        in_specs=(cube,) * 5 + (P("gx", "gy"),), out_specs=(cube,) * 5, check_vma=False)
```

```python
import functools

import jax
import jax.numpy as jnp
from jax import lax
from jax.experimental import pallas as pl
from jax.experimental.pallas import tpu as pltpu
from jax.sharding import PartitionSpec as P

ITERS = 3
STIFF = 30.0
PAD = 8
ROWS = 16
PARTS = 2
UNROLL = 24


def roll(value, shift):
    if isinstance(shift, int):
        shift = shift % value.shape[1]
    return pltpu.roll(value, shift, 1)


def kernel(n, ni, nj, sizes, east_in, north_in, vert_in, geo_in, press_in, mass,
           east, north, vert, geo, press,
           pp, up, psum, dvg, mu_s, c_s, planes, bounds,
           row_out, row_in, col_out, col_in, z_out, z_in,
           load_sem, row_send, row_recv, col_send, col_recv, z_send, z_recv):
    nx, ny, nz = sizes
    unroll = max(u for u in range(2, UNROLL + 1) if n % u == 0 and u % 2 == 0)
    ix, iy, iz = lax.axis_index("gx"), lax.axis_index("gy"), lax.axis_index("gz")
    xs = (lax.rem(ix + nx - 1, nx), lax.rem(ix + 1, nx))
    ys = (lax.rem(iy + ny - 1, ny), lax.rem(iy + 1, ny))

    loads = [
        pltpu.make_async_copy(press_in, pp.at[:, pl.ds(PAD, ni), :], load_sem.at[0]),
        pltpu.make_async_copy(east_in, up.at[:, pl.ds(PAD, ni), :], load_sem.at[1]),
        pltpu.make_async_copy(north_in, north, load_sem.at[2]),
        pltpu.make_async_copy(vert_in, vert, load_sem.at[3]),
        pltpu.make_async_copy(geo_in, geo, load_sem.at[4]),
    ]
    for load in loads:
        load.start()

    barrier = pltpu.get_barrier_semaphore()
    for t in range(2):
        pl.semaphore_signal(barrier, inc=1, device_id={"gx": xs[t]})
        pl.semaphore_signal(barrier, inc=1, device_id={"gy": ys[t]})
    for d in range(1, nz):
        pl.semaphore_signal(barrier, inc=1, device_id={"gz": lax.rem(iz + d, nz)})
    pl.semaphore_wait(barrier, 4 + nz - 1)

    def row_copy(slot, t):
        return pltpu.make_async_remote_copy(
            src_ref=row_out.at[slot, t], dst_ref=row_in.at[slot, 1 - t],
            send_sem=row_send.at[slot, t], recv_sem=row_recv.at[slot, 1 - t],
            device_id={"gx": xs[t]})

    span = ni // PARTS

    def part_rows(h):
        return pl.ds(pl.multiple_of(h * span, span), span)

    def col_copy(slot, t, h):
        return pltpu.make_async_remote_copy(
            src_ref=col_out.at[slot, t, part_rows(h), :], dst_ref=col_in.at[slot, 1 - t, part_rows(h), :],
            send_sem=col_send.at[slot, t, h], recv_sem=col_recv.at[slot, 1 - t, h],
            device_id={"gy": ys[t]})

    def z_copy(slot, d, h):
        return pltpu.make_async_remote_copy(
            src_ref=z_out.at[slot, :, part_rows(h), :], dst_ref=z_in.at[slot, d - 1, :, part_rows(h), :],
            send_sem=z_send.at[slot, d - 1, h], recv_sem=z_recv.at[slot, d - 1, h],
            device_id={"gz": lax.rem(iz + d, nz)})

    lane = lax.broadcasted_iota(jnp.int32, (ROWS, nj), 1)
    pair = lane // 2

    def merged(left, right, width):
        left, right = roll(left, width), roll(right, nj - width)
        even = pair % 2 == 0
        return jnp.where(even, right, left), jnp.where(even, left, right)

    def send_rows(slot, ref):
        row_out[slot, 0] = ref[:, PAD : PAD + 2, :]
        row_out[slot, 1] = ref[:, PAD + ni - 2 : PAD + ni, :]
        for t in range(2):
            row_copy(slot, t).start()

    def recv_rows(slot, ref):
        for t in range(2):
            row_copy(slot, t).wait()
        ref[:, PAD - 2 : PAD, :] = row_in[slot, 0]
        ref[:, PAD + ni : PAD + ni + 2, :] = row_in[slot, 1]

    def packed(value, k, packs):
        turned = roll(value, 2 * k + 2)
        return (jnp.where(pair == k + 1, turned, packs[0]), jnp.where(pair == k, turned, packs[1]))

    def strips(body, h=None):
        count = (ni if h is None else span) // ROWS
        first = 0 if h is None else h * count

        @pl.loop(0, count)
        def _(s):
            body(pl.multiple_of((first + s) * ROWS, ROWS))

    def send_cols(slot, load_level):
        def body(r0):
            zero = jnp.zeros((ROWS, nj), jnp.float32)

            def group(q, packs):
                for e in range(unroll):
                    k = q * unroll + e
                    packs = packed(load_level(k, r0), k, packs)
                return packs

            packs = lax.fori_loop(0, n // unroll, group, (zero, zero))
            for t in range(2):
                col_out[slot, t, pl.ds(r0, ROWS), :] = packs[t]

        strips(body)
        for h in range(PARTS):
            for t in range(2):
                col_copy(slot, t, h).start()

    loads[0].wait()
    send_rows(0, pp)
    send_cols(0, lambda k, r0: pp[k, pl.ds(PAD + r0, ROWS), :])
    loads[1].wait()
    send_rows(ITERS, up)
    loads[2].wait()
    send_cols(ITERS, lambda k, r0: north[k, pl.ds(r0, ROWS), :])

    stiff = STIFF * mass[...]
    root = jnp.sqrt(1.0 + 4.0 * stiff)
    major = 0.5 * (1.0 + 2.0 * stiff + root)
    mu_s[...] = stiff / major
    c_s[...] = 1.0 / major
    planes[0] = jnp.log(stiff / major)
    planes[1] = major / root
    planes[2] = major / stiff

    recv_rows(0, pp)
    recv_rows(ITERS, up)
    for slot in (0, ITERS):
        for t in range(2):
            for h in range(PARTS):
                col_copy(slot, t, h).wait()
    loads[3].wait()
    loads[4].wait()

    def pass_one(it, h):
        def body(r0):
            rows = pl.ds(r0, ROWS)
            m, mu, c = mass[rows, :], mu_s[rows, :], c_s[rows, :]
            weak, strong = 0.05 * m, 0.2 * m
            left, right = col_in[it, 0, rows, :], col_in[it, 1, rows, :]
            ends = merged(left, right, 2)
            if it == 0:
                vends = merged(col_in[ITERS, 0, rows, :], col_in[ITERS, 1, rows, :], 1)

            def star(k, parity):
                end = roll(ends[parity], nj - 2 - 2 * k)
                at = pl.ds(PAD + r0, ROWS)
                p = pp[k, at, :]
                low = jnp.where(lane < 2, end, roll(p, 2))
                high = jnp.where(lane >= nj - 2, end, roll(p, nj - 2))
                total = (pp[k, pl.ds(PAD + r0 + 2, ROWS), :] + pp[k, pl.ds(PAD + r0 - 2, ROWS), :]) + (low + high) - 4.0 * p
                if it == 0:
                    v = north[k, rows, :]
                    vend = roll(vends[parity], nj - 2 - 2 * k)
                    vlow = jnp.where(lane < 1, vend, roll(v, 1))
                    vhigh = jnp.where(lane >= nj - 1, vend, roll(v, nj - 1))
                    d = strong * (up[k, pl.ds(PAD + r0 + 1, ROWS), :] - up[k, pl.ds(PAD + r0 - 1, ROWS), :] + (vhigh - vlow))
                    psum[k, at, :] = p
                else:
                    d = dvg[k, rows, :]
                    psum[k, at, :] = psum[k, at, :] + p
                d = d - weak * total
                if it < ITERS - 1:
                    dvg[k, rows, :] = d
                ps = p - d
                press[k, rows, :] = ps
                return ps

            def sweep(k, above, below, state):
                y, dn, weight = state
                f = c * (vert[k, rows, :] + 0.5 * geo[k, rows, :] - (above - below))
                y = mu * y + f
                vert[k, rows, :] = y
                return y, dn + weight * f, weight * mu

            def steps(ks, carry):
                older, newer, state = carry
                for e, k in enumerate(ks):
                    ps = star(k, e % 2)
                    if not (isinstance(k, int) and k == 0):
                        state = sweep(k - 1, ps, older, state)
                    older, newer = newer, ps
                return older, newer, state

            zero = jnp.zeros((ROWS, nj), jnp.float32)
            carry = (zero, zero, (zero, zero, zero + 1.0))
            carry = steps(range(unroll), carry)
            planes_lo = press[0, rows, :]

            def group(q, carry):
                return steps([q * unroll + e for e in range(unroll)], carry)

            older, newer, state = lax.fori_loop(1, n // unroll, group, carry)
            y, dn, _ = sweep(n - 1, zero, older, state)
            z_out[it, 0, rows, :] = y
            z_out[it, 1, rows, :] = dn
            z_out[it, 2, rows, :] = c * planes_lo
            z_out[it, 3, rows, :] = c * newer

        strips(body, h)

    def interface(it, h):
        def body(r0):
            rows = pl.ds(r0, ROWS)
            mu, logmu, kappa, inv = mu_s[rows, :], planes[0, rows, :], planes[1, rows, :], planes[2, rows, :]
            zero = jnp.zeros((ROWS, nj), jnp.float32)

            def power(m):
                if not isinstance(m, int):
                    m = jnp.maximum(m, 0).astype(jnp.float32)
                return jnp.exp(m * logmu)

            near = power(n - 1)
            below, above, to_low, to_high = zero, zero, zero, zero
            pieces = {}

            def piece(d, which):
                if abs(d) >= nz:
                    return zero
                if d == 0:
                    return z_out[it, which, rows, :]
                value = z_in[it, (nz - d - 1) % nz if d > 0 else -d - 1, which, rows, :]
                inside = jnp.logical_and(iz + d >= 0, iz + d < nz)
                return jnp.where(inside, value, 0.0)

            own_up = own_dn = zero
            for d in range(-(nz - 1), nz):
                j = iz + d
                inside = jnp.logical_and(j >= 0, j < nz)
                under, over = piece(d - 1, 3), piece(d + 1, 2)
                upt = piece(d, 0) + near * under - over
                dnt = piece(d, 1) + under - near * over
                if d == 0:
                    own_up, own_dn = upt, dnt
                    delta_low, delta_high = under, over
                elif d < 0:
                    below = below + jnp.where(inside, power(n * (-1 - d)) * upt, 0.0)
                else:
                    above = above + jnp.where(inside, power(n * (d - 1)) * dnt, 0.0)
                to_low = to_low + jnp.where(inside, power(n * j + 1) * dnt, 0.0)
                to_high = to_high + jnp.where(inside, power(n * (nz - 1 - j) + 1) * upt, 0.0)
            q = power(n * nz + 1)
            scale = kappa / (1.0 - q * q)
            alpha = kappa * below + (q * to_high - to_low) * scale * power(n * iz)
            beta = kappa * above + (q * to_low - to_high) * scale * power(n * (nz - 1 - iz))
            far = power(n + 1)
            bounds[2, rows, :] = kappa * mu * own_dn + alpha + beta * far
            bounds[3, rows, :] = kappa * mu * own_up + beta + alpha * far
            alpha = alpha + kappa * delta_low * inv
            beta = beta - kappa * delta_high * inv
            bounds[0, rows, :] = kappa * mu * z_out[it, 0, rows, :] + beta
            bounds[1, rows, :] = alpha * power(n)

        strips(body, h)

    def pass_two(it, h):
        last = it == ITERS - 1

        def body(r0):
            rows = pl.ds(r0, ROWS)
            mu, inv = mu_s[rows, :], planes[2, rows, :]
            half = 0.5 * mass[rows, :]
            zero = jnp.zeros((ROWS, nj), jnp.float32)

            def finish(k, above, below, packs):
                p = press[k, rows, :] - half * (above - below)
                if last:
                    press[k, rows, :] = p
                    return packs
                pp[k, pl.ds(PAD + r0, ROWS), :] = p
                return packed(p, k, packs)

            def steps(ks, carry):
                x, h, older, newer, packs = carry
                for k in ks:
                    x = mu * x + vert[k, rows, :]
                    v = x + h
                    h = h * inv
                    vert[k, rows, :] = v
                    geo[k, rows, :] = geo[k, rows, :] + 0.5 * v
                    if not (isinstance(k, int) and k == n - 1):
                        packs = finish(k + 1, older, v, packs)
                    older, newer = newer, v
                return x, h, older, newer, packs

            top = bounds[3, rows, :]
            carry = (bounds[0, rows, :], bounds[1, rows, :], zero, top, (zero, zero))
            carry = steps([n - 1 - e for e in range(unroll)], carry)

            def group(q, carry):
                return steps([n - 1 - q * unroll - e for e in range(unroll)], carry)

            _, _, older, newer, packs = lax.fori_loop(1, n // unroll, group, carry)
            packs = finish(0, older, bounds[2, rows, :], packs)
            if not last:
                for t in range(2):
                    col_out[it + 1, t, rows, :] = packs[t]

        strips(body, h)

    def winds():
        def body(r0):
            rows = pl.ds(r0, ROWS)
            left = col_in[0, 0, rows, :]
            right = col_in[0, 1, rows, :]
            for it in range(1, ITERS):
                left = left + col_in[it, 0, rows, :]
                right = right + col_in[it, 1, rows, :]

            ends = merged(left, right, 1)

            def group(q, carry):
                for e in range(unroll):
                    k = q * unroll + e
                    end = roll(ends[e % 2], nj - 2 - 2 * k)
                    at = pl.ds(PAD + r0, ROWS)
                    p = psum[k, at, :]
                    east[k, rows, :] = up[k, at, :] - 0.25 * (
                        psum[k, pl.ds(PAD + r0 + 1, ROWS), :] - psum[k, pl.ds(PAD + r0 - 1, ROWS), :])
                    low = jnp.where(lane < 1, end, roll(p, 1))
                    high = jnp.where(lane >= nj - 1, end, roll(p, nj - 1))
                    north[k, rows, :] = north[k, rows, :] - 0.25 * (high - low)
                return carry

            lax.fori_loop(0, n // unroll, group, 0)

        strips(body)

    for it in range(ITERS):
        if it > 0:
            recv_rows(it, pp)

        @pl.loop(0, PARTS)
        def _(h, it=it):
            if it > 0:
                for t in range(2):
                    col_copy(it, t, h).wait()
            pass_one(it, h)
            for d in range(1, nz):
                z_copy(it, d, h).start()

        if it == ITERS - 1:
            for t, at in ((0, PAD - 2), (1, PAD + ni)):
                total = row_in[0, t]
                for slot in range(1, ITERS):
                    total = total + row_in[slot, t]
                psum[:, at : at + 2, :] = total
            winds()

        @pl.loop(0, PARTS)
        def _(h, it=it):
            for d in range(1, nz):
                z_copy(it, d, h).wait()
            interface(it, h)
            pass_two(it, h)
            if it < ITERS - 1:
                for t in range(2):
                    col_copy(it + 1, t, h).start()

        if it < ITERS - 1:
            send_rows(it + 1, pp)


def local(sizes, east, north, vert, geo, press, mass):
    n, ni, nj = east.shape
    nz = sizes[2]
    f32 = jnp.float32
    slots = ITERS + 1
    field = pltpu.VMEM((n, ni, nj), f32)
    padded = pltpu.VMEM((n, ni + 2 * PAD, nj), f32)
    plane = pltpu.VMEM((ni, nj), f32)
    return pl.pallas_call(
        functools.partial(kernel, n, ni, nj, sizes),
        out_shape=[pltpu.VMEM((n, ni, nj), f32)] * 5,
        in_specs=[pl.BlockSpec(memory_space=pl.ANY)] * 5 + [pl.BlockSpec(memory_space=pltpu.VMEM)],
        out_specs=[pl.BlockSpec(memory_space=pltpu.VMEM)] * 5,
        scratch_shapes=[
            padded, padded, padded, field, plane, plane,
            pltpu.VMEM((3, ni, nj), f32),
            pltpu.VMEM((4, ni, nj), f32),
            pltpu.VMEM((slots, 2, n, 2, nj), f32),
            pltpu.VMEM((slots, 2, n, 2, nj), f32),
            pltpu.VMEM((slots, 2, ni, nj), f32),
            pltpu.VMEM((slots, 2, ni, nj), f32),
            pltpu.VMEM((ITERS, 4, ni, nj), f32),
            pltpu.VMEM((ITERS, nz - 1, 4, ni, nj), f32),
            pltpu.SemaphoreType.DMA((5,)),
            pltpu.SemaphoreType.DMA((slots, 2)),
            pltpu.SemaphoreType.DMA((slots, 2)),
            pltpu.SemaphoreType.DMA((slots, 2, PARTS)),
            pltpu.SemaphoreType.DMA((slots, 2, PARTS)),
            pltpu.SemaphoreType.DMA((ITERS, nz - 1, PARTS)),
            pltpu.SemaphoreType.DMA((ITERS, nz - 1, PARTS)),
        ],
        compiler_params=pltpu.CompilerParams(
            collective_id=0, has_side_effects=True, vmem_limit_bytes=40 * 1024 * 1024),
    )(east, north, vert, geo, press, mass)


LAG = 5
TILE = 16
WIDE = 32


def paired(n, ni, nj, sizes, east_in, north_in, vert_in, geo_in, press_in, mass_in,
           rhs, star, geo, coef, p0, up, north, edge, faces,
           p1, p2, dvg, head, turned_a, turned_b, turned_c, side, mass, con, packs_p, packs_v,
           row_out, row_in, col_out, col_in, z_out, z_in,
           load_sem, sent, row_recv, col_recv, z_recv):
    nx, ny, _ = sizes
    per = nj // 4
    count = ni // TILE
    press = (p0, p1, p2)
    turned = (turned_a, turned_c, turned_a)
    ix, iy, iz = lax.axis_index("gx"), lax.axis_index("gy"), lax.axis_index("gz")
    xs = (lax.rem(ix + nx - 1, nx), lax.rem(ix + 1, nx))
    ys = (lax.rem(iy + ny - 1, ny), lax.rem(iy + 1, ny))
    flip = (1 - 2 * iz).astype(jnp.float32)
    half = 0.5 * flip
    inner = pl.ds(PAD, ni)

    barrier = pltpu.get_barrier_semaphore()
    for t in range(2):
        pl.semaphore_signal(barrier, inc=1, device_id={"gx": xs[t]})
        pl.semaphore_signal(barrier, inc=1, device_id={"gy": ys[t]})
    pl.semaphore_signal(barrier, inc=1, device_id={"gz": 1 - iz})

    mass_load = pltpu.make_async_copy(mass_in, mass, load_sem.at[5])
    mass_load.start()
    fields = (
        (press_in, p0.at[:, inner, :]), (north_in, north), (east_in, up.at[:, inner, :]),
        (vert_in, head), (geo_in, geo))

    def load(e, m):
        src, dst = fields[e]
        k = iz * (n - 1) + (1 - 2 * iz) * m
        pltpu.make_async_copy(src.at[k], dst.at[m], load_sem.at[e]).start()

    def loaded(e):
        pltpu.make_async_copy(fields[e][0], fields[e][1], load_sem.at[e]).wait()

    @pl.loop(0, n)
    def _(m):
        load(0, m)

    def row_copy(it, t):
        return pltpu.make_async_remote_copy(
            src_ref=row_out.at[it, t], dst_ref=row_in.at[it, 1 - t],
            send_sem=sent.at[0], recv_sem=row_recv.at[it],
            device_id={"gx": xs[t]})

    def arrived(out, inn, e, sem, axis):
        pltpu.make_async_remote_copy(
            src_ref=out, dst_ref=inn, send_sem=sent.at[e], recv_sem=sem,
            device_id={axis: 1 - iz if axis == "gz" else xs[0] if axis == "gx" else ys[0]}).wait_recv()

    def rows_of(s):
        return pl.ds(pl.multiple_of(s * TILE, TILE), TILE)

    def col_copy(it, t, s):
        return pltpu.make_async_remote_copy(
            src_ref=col_out.at[it, t, rows_of(s), :], dst_ref=col_in.at[it, 1 - t, rows_of(s), :],
            send_sem=sent.at[1], recv_sem=col_recv.at[it, s],
            device_id={"gy": ys[t]})

    def z_copy(it, s):
        return pltpu.make_async_remote_copy(
            src_ref=z_out.at[it, :, rows_of(s), :], dst_ref=z_in.at[it, :, rows_of(s), :],
            send_sem=sent.at[2], recv_sem=z_recv.at[it, s],
            device_id={"gz": 1 - iz})

    lane = lax.broadcasted_iota(jnp.int32, (TILE, nj), 1)
    part, couple, quad = lane % 4, lane // 2, lane // 4
    zero = jnp.zeros((TILE, nj), jnp.float32)
    whole = lax.broadcasted_iota(jnp.int32, (ni, nj), 1) % 4

    def placed(mask, value, m, packs):
        b = m // per
        return tuple(jnp.where(mask, value, packs[c]) if c == b else packs[c] for c in range(2))

    def outgoing(it, rows, part, packs):
        a, b = packs
        col_out[it, 0, rows, :] = jnp.where(part >= 2, a, roll(b, -2))
        col_out[it, 1, rows, :] = jnp.where(part < 2, a, roll(b, 2))

    mass_load.wait()
    inverse = 1.0 / (STIFF * mass[...])
    con[0] = 1.25 * inverse
    con[1] = 0.25 * inverse
    base = 2.0 + inverse

    def pivot(m, a):
        load(1, m)
        a = 1.0 / (base - a)
        coef[m] = a
        return a

    last = lax.fori_loop(0, n, pivot, jnp.zeros((ni, nj), jnp.float32))
    con[2] = last / (1.0 - last * last)

    wide = lax.broadcasted_iota(jnp.int32, (WIDE, nj), 1)
    blank = jnp.zeros((WIDE, nj), jnp.float32)
    share = n * WIDE // ni

    loaded(0)

    @pl.loop(0, ni // WIDE)
    def _(b):
        r0 = pl.multiple_of(b * WIDE, WIDE)
        rows = pl.ds(r0, WIDE)
        packs = (blank, blank)
        for m in range(n):
            value = roll(p0[m, pl.ds(PAD + r0, WIDE), :], 4 * (m % per) + 2)
            turned_a[m, rows, :] = value
            packs = placed(wide // 4 == m % per, value, m, packs)
            if m < share:
                load(2, b * share + m)
        packs_p[0, rows, :], packs_p[1, rows, :] = packs

    loaded(1)

    @pl.loop(0, ni // WIDE)
    def _(b):
        r0 = pl.multiple_of(b * WIDE, WIDE)
        rows = pl.ds(r0, WIDE)
        packs = (blank, blank)
        for m in range(n):
            q = 4 * (m % per)
            value = roll(4.0 * north[m, rows, :], q + 1)
            turned_b[m, rows, :] = turned_a[m, rows, :] + value
            packs = placed(wide // 2 == q // 2, value, m, packs)
            if m < share:
                load(3, b * share + m)
                load(4, b * share + m)
        packs_v[0, rows, :], packs_v[1, rows, :] = packs

    edges = []
    for c in range(2):
        v = packs_v[c]
        back = roll(v, 2)
        edges.append(packs_p[c] + jnp.where(whole == 0, v, jnp.where(whole == 3, -back, 0.0)))
        packs_v[c] = jnp.where(whole == 1, v, jnp.where(whole == 2, -back, 0.0))
    outgoing(0, slice(None), whole, edges)

    pl.semaphore_wait(barrier, 5)

    @pl.loop(0, count)
    def _(t):
        s = lax.rem(t + 1, count)
        for t in range(2):
            col_copy(0, t, s).start()

    loaded(2)
    up[:, :PAD, :] = jnp.zeros((n, PAD, nj), jnp.float32)
    up[:, PAD + ni :, :] = jnp.zeros((n, PAD, nj), jnp.float32)
    row_out[0, 0] = p0[:, PAD : PAD + 2, :] - 4.0 * up[:, PAD - 1 : PAD + 1, :]
    row_out[0, 1] = p0[:, PAD + ni - 2 : PAD + ni, :] + 4.0 * up[:, PAD + ni - 1 : PAD + ni + 1, :]
    for t in range(2):
        row_copy(0, t).start()

    @pl.loop(0, ni // WIDE)
    def _(b):
        rows = pl.ds(pl.multiple_of(b * WIDE, WIDE), WIDE)
        for m in range(n):
            turned_a[m, rows, :] = turned_a[m, rows, :] - roll(4.0 * north[m, rows, :], 4 * (m % per) + 3)

    loaded(3)
    loaded(4)

    def lateral(it, s):
        rows = rows_of(s)
        left, right = col_in[it, 0, rows, :], col_in[it, 1, rows, :]
        ends = (jnp.where(part < 2, left, right), jnp.where(part < 2, roll(left, -2), roll(right, 2)))
        if it == 0:
            ends = [ends[c] + packs_v[c, rows, :] for c in range(2)]

        def level(m):
            q, end = m % per, ends[m // per]
            lower = upper = turned[it][m, rows, :]
            if it == 0:
                lower = turned_b[m, rows, :]
            low = roll(jnp.where(couple == 2 * q, end, lower), -4 * q)
            high = roll(jnp.where(couple == 2 * q + 1, end, upper), -4 * q - 4)
            side[m] = low + high

        return level

    def forward(it, s):
        rows = rows_of(s)
        r0 = PAD + pl.multiple_of(s * TILE, TILE)
        at = pl.ds(r0, TILE)
        weak = 0.05 * mass[rows, :]
        four = 4.0 * weak
        state = {"older": zero, "newer": None, "g": None}

        def close(m, above):
            own = head[m, rows, :]
            if it == 0:
                own = flip * own + half * geo[m, rows, :]
            g = own - (above - state["older"])
            if m > 0:
                g = g + coef[m - 1, rows, :] * state["g"]
            rhs[m, rows, :] = g
            state["g"] = g

        def level(m):
            ref = press[it]
            p = ref[m, at, :]
            total = (ref[m, pl.ds(r0 + 2, TILE), :] + ref[m, pl.ds(r0 - 2, TILE), :]) + side[m]
            d = four * p
            if it == 0:
                total = total - 4.0 * (up[m, pl.ds(r0 + 1, TILE), :] - up[m, pl.ds(r0 - 1, TILE), :])
            else:
                d = dvg[m, rows, :] + d
            d = d - weak * total
            if it < ITERS - 1:
                dvg[m, rows, :] = d
            else:
                p0[m, at, :] = (p0[m, at, :] + p1[m, at, :]) + p
            ps = p - d
            star[m, rows, :] = ps
            if m > 0:
                close(m - 1, ps)
                state["older"] = state["newer"]
            state["newer"] = ps

        def finish():
            close(n - 1, zero)
            z_out[it, 0, rows, :] = state["g"]
            z_out[it, 1, rows, :] = state["newer"]
            z_copy(it, s).start()

        return level, finish

    def col_wait(it, s):
        arrived(col_out.at[it, :, rows_of(s), :], col_in.at[it, :, rows_of(s), :], 1, col_recv.at[it, s], "gy")

    def row_wait(it):
        arrived(row_out.at[it], row_in.at[it], 0, row_recv.at[it], "gx")
        press[it][:, PAD - 2 : PAD, :] = row_in[it, 0]
        press[it][:, PAD + ni : PAD + ni + 2, :] = row_in[it, 1]

    def meet(a, w, out, inn):
        mine, other = out[0] - inn[1], inn[0] - out[1]
        z = w * (mine - a * other)
        return z, a * (z - other)

    def backward(it, s):
        rows = rows_of(s)
        at = pl.ds(PAD + pl.multiple_of(s * TILE, TILE), TILE)
        near, far = con[0, rows, :], con[1, rows, :]
        z_copy(it, s).wait_recv()
        state = {"packs": (zero, zero)}
        state["z"], state["above"] = meet(
            coef[n - 1, rows, :], con[2, rows, :],
            [z_out[it, c, rows, :] for c in range(2)], [z_in[it, c, rows, :] for c in range(2)])

        def level(m):
            z = state["z"]
            g = geo[m, rows, :]
            if it == 0:
                g = half * g
            head[m, rows, :] = near * z + g
            geo[m, rows, :] = far * z + g
            below = coef[m - 1, rows, :] * (rhs[m - 1, rows, :] + z) if m > 0 else zero
            p = star[m, rows, :] - (0.5 / STIFF) * (state["above"] - below)
            press[it + 1][m, at, :] = p
            value = roll(p, 4 * (m % per) + 2)
            turned[it + 1][m, rows, :] = value
            state["packs"] = placed(quad == m % per, value, m, state["packs"])
            state["above"], state["z"] = z, below

        def finish():
            outgoing(it + 1, rows, part, state["packs"])
            for t in range(2):
                col_copy(it + 1, t, s).start()

        return level, finish

    for it in range(ITERS):
        final = it == ITERS - 1
        front = (count - 2, count - 2, count - 2)[it]
        lag = count if final else LAG

        def order(t, front=front):
            return jnp.where(t < front, t + 1, jnp.where(t == front, count - 1, jnp.where(t == front + 1, 0, t - 1)))

        def ahead_of(t, it=it, front=front, order=order):
            @pl.when(t == front)
            def _():
                row_wait(it)

            after = order(lax.rem(t + 1, count))

            @pl.when(t < count - 1)
            def _():
                col_wait(it, after)

            return forward(it, order(t)) + (lateral(it, after),)

        def behind(u, it=it, order=order):
            return backward(it, order(u))

        def send_rows(u, it=it, front=front):
            @pl.when(u == front)
            def _():
                row_out[it + 1, 1] = press[it + 1][:, PAD + ni - 2 : PAD + ni, :]
                row_copy(it + 1, 1).start()

            @pl.when(u == front + 1)
            def _():
                row_out[it + 1, 0] = press[it + 1][:, PAD : PAD + 2, :]
                row_copy(it + 1, 0).start()

        col_wait(it, order(0))
        first = lateral(it, order(0))
        for m in range(n):
            first(m)

        @pl.loop(0, lag)
        def _(t):
            one, finish, ahead = ahead_of(t)
            for m in range(n):
                one(m)
                ahead(m)
            finish()

        if not final:
            @pl.loop(lag, count)
            def _(t):
                one, finish, ahead = ahead_of(t)
                for m in range(n):
                    one(m)
                    ahead(m)
                finish()
                two, deliver = behind(t - lag)
                for m in range(n):
                    two(n - 1 - m)
                deliver()
                send_rows(t - lag)

            @pl.loop(count - lag, count)
            def _(u):
                two, deliver = behind(u)
                for m in range(n):
                    two(n - 1 - m)
                deliver()
                send_rows(u)

    for t, at in ((0, PAD - 2), (1, PAD + ni)):
        p0[:, at : at + 2, :] = (row_in[0, t] + row_in[1, t]) + row_in[2, t]
    left = (col_in[0, 0] + col_in[1, 0]) + col_in[2, 0]
    right = (col_in[0, 1] + col_in[1, 1]) + col_in[2, 1]
    edge[0] = jnp.where(whole == 1, roll(right, -1), roll(left, 1))
    edge[1] = jnp.where(whole == 1, roll(right, 1), roll(left, -1))

    @pl.loop(0, count)
    def _(s):
        z_copy(ITERS - 1, s).wait_recv()

    faces[0], faces[1] = meet(
        coef[n - 1], con[2], [z_out[ITERS - 1, c] for c in range(2)], [z_in[ITERS - 1, c] for c in range(2)])

    for e, out, inn, axis in ((0, row_out, row_in, "gx"), (1, col_out, col_in, "gy"), (2, z_out, z_in, "gz")):
        pltpu.make_async_remote_copy(
            src_ref=out, dst_ref=inn, send_sem=sent.at[e], recv_sem=load_sem.at[e],
            device_id={axis: 1 - iz if axis == "gz" else xs[0] if axis == "gx" else ys[0]}).wait_send()


def finale(n, ni, nj, rhs, star, geo, coef, psum, up, north, edge, faces, mass,
           east_out, north_out, vert_out, geo_out, press_out,
           east_s, north_s, vert_s, geo_s, press_s, sem):
    per = nj // 4
    count = ni // WIDE
    iz = lax.axis_index("gz")
    flip = (1 - 2 * iz).astype(jnp.float32)
    lane = lax.broadcasted_iota(jnp.int32, (WIDE, nj), 1)

    def store(e, src, dst, rows):
        return pltpu.make_async_copy(src.at[:, rows, :], dst.at[:, rows, :], sem.at[e])

    outs = ((east_s, east_out), (north_s, north_out), (vert_s, vert_out), (geo_s, geo_out), (press_s, press_out))

    def level_of(m):
        return iz * (n - 1) + (1 - 2 * iz) * m

    @pl.loop(0, count)
    def _(s):
        rows = pl.ds(pl.multiple_of(s * WIDE, WIDE), WIDE)
        v_of = flip / (STIFF * mass[rows, :])
        half = 0.5 * v_of
        twice = 2.0 * flip
        z, above = faces[0, rows, :], faces[1, rows, :]
        for m in range(n - 1, -1, -1):
            k = level_of(m)
            vert_s[k, rows, :] = v_of * z
            geo_s[k, rows, :] = twice * geo[m, rows, :] + half * z
            below = coef[m - 1, rows, :] * (rhs[m - 1, rows, :] + z) if m > 0 else jnp.zeros_like(z)
            press_s[k, rows, :] = star[m, rows, :] - (0.5 / STIFF) * (above - below)
            above, z = z, below
        for e in (2, 3, 4):
            store(e, *outs[e], rows).start()

    @pl.loop(0, count)
    def _(s):
        rows = pl.ds(pl.multiple_of(s * WIDE, WIDE), WIDE)
        r0 = PAD + pl.multiple_of(s * WIDE, WIDE)
        ends = (edge[0, rows, :], edge[1, rows, :])
        for m in range(n):
            k = level_of(m)
            p = psum[m, pl.ds(r0, WIDE), :]
            end = roll(ends[m // per], nj - 2 - 4 * (m % per))
            low = jnp.where(lane < 1, end, roll(p, 1))
            high = jnp.where(lane >= nj - 1, end, roll(p, nj - 1))
            north_s[k, rows, :] = north[m, rows, :] - 0.25 * (high - low)
            east_s[k, rows, :] = up[m, pl.ds(r0, WIDE), :] - 0.25 * (
                psum[m, pl.ds(r0 + 1, WIDE), :] - psum[m, pl.ds(r0 - 1, WIDE), :])
        for e in (0, 1):
            store(e, *outs[e], rows).start()

    for e in range(5):
        pltpu.make_async_copy(outs[e][0], outs[e][1], sem.at[e]).wait()


def pair(sizes, east, north, vert, geo, press, mass):
    n, ni, nj = east.shape
    f32 = jnp.float32
    count = ni // TILE
    shape = (n, ni, nj)
    padded = (n, ni + 2 * PAD, nj)
    kept = [shape, shape, shape, shape, padded, padded, shape, (2, ni, nj), (2, ni, nj)]
    vmem = pl.BlockSpec(memory_space=pltpu.VMEM)
    state = pl.pallas_call(
        functools.partial(paired, n, ni, nj, sizes),
        out_shape=[pltpu.VMEM(s, f32) for s in kept],
        in_specs=[pl.BlockSpec(memory_space=pltpu.HBM)] * 6,
        out_specs=[vmem] * len(kept),
        scratch_shapes=[
            pltpu.VMEM(padded, f32), pltpu.VMEM(padded, f32), pltpu.VMEM(shape, f32), pltpu.VMEM(shape, f32),
            pltpu.VMEM(shape, f32), pltpu.VMEM(shape, f32), pltpu.VMEM(shape, f32),
            pltpu.VMEM((n, TILE, nj), f32),
            pltpu.VMEM((ni, nj), f32),
            pltpu.VMEM((3, ni, nj), f32),
            pltpu.VMEM((2, ni, nj), f32),
            pltpu.VMEM((2, ni, nj), f32),
            pltpu.VMEM((ITERS, 2, n, 2, nj), f32),
            pltpu.VMEM((ITERS, 2, n, 2, nj), f32),
            pltpu.VMEM((ITERS, 2, ni, nj), f32),
            pltpu.VMEM((ITERS, 2, ni, nj), f32),
            pltpu.VMEM((ITERS, 2, ni, nj), f32),
            pltpu.VMEM((ITERS, 2, ni, nj), f32),
            pltpu.SemaphoreType.DMA((6,)),
            pltpu.SemaphoreType.DMA((3,)),
            pltpu.SemaphoreType.DMA((ITERS,)),
            pltpu.SemaphoreType.DMA((ITERS, count)),
            pltpu.SemaphoreType.DMA((ITERS, count)),
        ],
        compiler_params=pltpu.CompilerParams(
            collective_id=0, has_side_effects=True, vmem_limit_bytes=41 * 1024 * 1024),
    )(east, north, vert, geo, press, mass)
    return pl.pallas_call(
        functools.partial(finale, n, ni, nj),
        out_shape=[jax.ShapeDtypeStruct(shape, f32)] * 5,
        in_specs=[vmem] * (len(kept) + 1),
        out_specs=[pl.BlockSpec(memory_space=pl.ANY)] * 5,
        scratch_shapes=[pltpu.VMEM(shape, f32)] * 5 + [pltpu.SemaphoreType.DMA((5,))],
        compiler_params=pltpu.CompilerParams(vmem_limit_bytes=18 * 1024 * 1024),
    )(*state, mass)


def solution(mesh):
    sizes = (mesh.shape["gx"], mesh.shape["gy"], mesh.shape["gz"])
    cube = P("gz", "gx", "gy")

    def body(east, *rest):
        n, ni, nj = east.shape
        fits = sizes[2] == 2 and n <= nj // 2 and ni % TILE == 0 and ni // TILE > LAG and ni % WIDE == 0 and n * WIDE % ni == 0 and ITERS == 3
        return (pair if fits else local)(sizes, east, *rest)

    return jax.shard_map(
        body, mesh=mesh,
        in_specs=(cube,) * 5 + (P("gx", "gy"),), out_specs=(cube,) * 5, check_vma=False)
```

```python
import functools

import jax
import jax.numpy as jnp
from jax import lax
from jax.experimental import pallas as pl
from jax.experimental.pallas import tpu as pltpu
from jax.sharding import PartitionSpec as P

ITERS = 3
STIFF = 30.0
PAD = 8
ROWS = 16
PARTS = 2
UNROLL = 24


def roll(value, shift):
    if isinstance(shift, int):
        shift = shift % value.shape[1]
    return pltpu.roll(value, shift, 1)


def kernel(n, ni, nj, sizes, east_in, north_in, vert_in, geo_in, press_in, mass,
           east, north, vert, geo, press,
           pp, up, psum, dvg, mu_s, c_s, planes, bounds,
           row_out, row_in, col_out, col_in, z_out, z_in,
           load_sem, row_send, row_recv, col_send, col_recv, z_send, z_recv):
    nx, ny, nz = sizes
    unroll = max(u for u in range(2, UNROLL + 1) if n % u == 0 and u % 2 == 0)
    ix, iy, iz = lax.axis_index("gx"), lax.axis_index("gy"), lax.axis_index("gz")
    xs = (lax.rem(ix + nx - 1, nx), lax.rem(ix + 1, nx))
    ys = (lax.rem(iy + ny - 1, ny), lax.rem(iy + 1, ny))

    loads = [
        pltpu.make_async_copy(press_in, pp.at[:, pl.ds(PAD, ni), :], load_sem.at[0]),
        pltpu.make_async_copy(east_in, up.at[:, pl.ds(PAD, ni), :], load_sem.at[1]),
        pltpu.make_async_copy(north_in, north, load_sem.at[2]),
        pltpu.make_async_copy(vert_in, vert, load_sem.at[3]),
        pltpu.make_async_copy(geo_in, geo, load_sem.at[4]),
    ]
    for load in loads:
        load.start()

    barrier = pltpu.get_barrier_semaphore()
    for t in range(2):
        pl.semaphore_signal(barrier, inc=1, device_id={"gx": xs[t]})
        pl.semaphore_signal(barrier, inc=1, device_id={"gy": ys[t]})
    for d in range(1, nz):
        pl.semaphore_signal(barrier, inc=1, device_id={"gz": lax.rem(iz + d, nz)})
    pl.semaphore_wait(barrier, 4 + nz - 1)

    def row_copy(slot, t):
        return pltpu.make_async_remote_copy(
            src_ref=row_out.at[slot, t], dst_ref=row_in.at[slot, 1 - t],
            send_sem=row_send.at[slot, t], recv_sem=row_recv.at[slot, 1 - t],
            device_id={"gx": xs[t]})

    span = ni // PARTS

    def part_rows(h):
        return pl.ds(pl.multiple_of(h * span, span), span)

    def col_copy(slot, t, h):
        return pltpu.make_async_remote_copy(
            src_ref=col_out.at[slot, t, part_rows(h), :], dst_ref=col_in.at[slot, 1 - t, part_rows(h), :],
            send_sem=col_send.at[slot, t, h], recv_sem=col_recv.at[slot, 1 - t, h],
            device_id={"gy": ys[t]})

    def z_copy(slot, d, h):
        return pltpu.make_async_remote_copy(
            src_ref=z_out.at[slot, :, part_rows(h), :], dst_ref=z_in.at[slot, d - 1, :, part_rows(h), :],
            send_sem=z_send.at[slot, d - 1, h], recv_sem=z_recv.at[slot, d - 1, h],
            device_id={"gz": lax.rem(iz + d, nz)})

    lane = lax.broadcasted_iota(jnp.int32, (ROWS, nj), 1)
    pair = lane // 2

    def merged(left, right, width):
        left, right = roll(left, width), roll(right, nj - width)
        even = pair % 2 == 0
        return jnp.where(even, right, left), jnp.where(even, left, right)

    def send_rows(slot, ref):
        row_out[slot, 0] = ref[:, PAD : PAD + 2, :]
        row_out[slot, 1] = ref[:, PAD + ni - 2 : PAD + ni, :]
        for t in range(2):
            row_copy(slot, t).start()

    def recv_rows(slot, ref):
        for t in range(2):
            row_copy(slot, t).wait()
        ref[:, PAD - 2 : PAD, :] = row_in[slot, 0]
        ref[:, PAD + ni : PAD + ni + 2, :] = row_in[slot, 1]

    def packed(value, k, packs):
        turned = roll(value, 2 * k + 2)
        return (jnp.where(pair == k + 1, turned, packs[0]), jnp.where(pair == k, turned, packs[1]))

    def strips(body, h=None):
        count = (ni if h is None else span) // ROWS
        first = 0 if h is None else h * count

        @pl.loop(0, count)
        def _(s):
            body(pl.multiple_of((first + s) * ROWS, ROWS))

    def send_cols(slot, load_level):
        def body(r0):
            zero = jnp.zeros((ROWS, nj), jnp.float32)

            def group(q, packs):
                for e in range(unroll):
                    k = q * unroll + e
                    packs = packed(load_level(k, r0), k, packs)
                return packs

            packs = lax.fori_loop(0, n // unroll, group, (zero, zero))
            for t in range(2):
                col_out[slot, t, pl.ds(r0, ROWS), :] = packs[t]

        strips(body)
        for h in range(PARTS):
            for t in range(2):
                col_copy(slot, t, h).start()

    loads[0].wait()
    send_rows(0, pp)
    send_cols(0, lambda k, r0: pp[k, pl.ds(PAD + r0, ROWS), :])
    loads[1].wait()
    send_rows(ITERS, up)
    loads[2].wait()
    send_cols(ITERS, lambda k, r0: north[k, pl.ds(r0, ROWS), :])

    stiff = STIFF * mass[...]
    root = jnp.sqrt(1.0 + 4.0 * stiff)
    major = 0.5 * (1.0 + 2.0 * stiff + root)
    mu_s[...] = stiff / major
    c_s[...] = 1.0 / major
    planes[0] = jnp.log(stiff / major)
    planes[1] = major / root
    planes[2] = major / stiff

    recv_rows(0, pp)
    recv_rows(ITERS, up)
    for slot in (0, ITERS):
        for t in range(2):
            for h in range(PARTS):
                col_copy(slot, t, h).wait()
    loads[3].wait()
    loads[4].wait()

    def pass_one(it, h):
        def body(r0):
            rows = pl.ds(r0, ROWS)
            m, mu, c = mass[rows, :], mu_s[rows, :], c_s[rows, :]
            weak, strong = 0.05 * m, 0.2 * m
            left, right = col_in[it, 0, rows, :], col_in[it, 1, rows, :]
            ends = merged(left, right, 2)
            if it == 0:
                vends = merged(col_in[ITERS, 0, rows, :], col_in[ITERS, 1, rows, :], 1)

            def star(k, parity):
                end = roll(ends[parity], nj - 2 - 2 * k)
                at = pl.ds(PAD + r0, ROWS)
                p = pp[k, at, :]
                low = jnp.where(lane < 2, end, roll(p, 2))
                high = jnp.where(lane >= nj - 2, end, roll(p, nj - 2))
                total = (pp[k, pl.ds(PAD + r0 + 2, ROWS), :] + pp[k, pl.ds(PAD + r0 - 2, ROWS), :]) + (low + high) - 4.0 * p
                if it == 0:
                    v = north[k, rows, :]
                    vend = roll(vends[parity], nj - 2 - 2 * k)
                    vlow = jnp.where(lane < 1, vend, roll(v, 1))
                    vhigh = jnp.where(lane >= nj - 1, vend, roll(v, nj - 1))
                    d = strong * (up[k, pl.ds(PAD + r0 + 1, ROWS), :] - up[k, pl.ds(PAD + r0 - 1, ROWS), :] + (vhigh - vlow))
                    psum[k, at, :] = p
                else:
                    d = dvg[k, rows, :]
                    psum[k, at, :] = psum[k, at, :] + p
                d = d - weak * total
                if it < ITERS - 1:
                    dvg[k, rows, :] = d
                ps = p - d
                press[k, rows, :] = ps
                return ps

            def sweep(k, above, below, state):
                y, dn, weight = state
                f = c * (vert[k, rows, :] + 0.5 * geo[k, rows, :] - (above - below))
                y = mu * y + f
                vert[k, rows, :] = y
                return y, dn + weight * f, weight * mu

            def steps(ks, carry):
                older, newer, state = carry
                for e, k in enumerate(ks):
                    ps = star(k, e % 2)
                    if not (isinstance(k, int) and k == 0):
                        state = sweep(k - 1, ps, older, state)
                    older, newer = newer, ps
                return older, newer, state

            zero = jnp.zeros((ROWS, nj), jnp.float32)
            carry = (zero, zero, (zero, zero, zero + 1.0))
            carry = steps(range(unroll), carry)
            planes_lo = press[0, rows, :]

            def group(q, carry):
                return steps([q * unroll + e for e in range(unroll)], carry)

            older, newer, state = lax.fori_loop(1, n // unroll, group, carry)
            y, dn, _ = sweep(n - 1, zero, older, state)
            z_out[it, 0, rows, :] = y
            z_out[it, 1, rows, :] = dn
            z_out[it, 2, rows, :] = c * planes_lo
            z_out[it, 3, rows, :] = c * newer

        strips(body, h)

    def interface(it, h):
        def body(r0):
            rows = pl.ds(r0, ROWS)
            mu, logmu, kappa, inv = mu_s[rows, :], planes[0, rows, :], planes[1, rows, :], planes[2, rows, :]
            zero = jnp.zeros((ROWS, nj), jnp.float32)

            def power(m):
                if not isinstance(m, int):
                    m = jnp.maximum(m, 0).astype(jnp.float32)
                return jnp.exp(m * logmu)

            near = power(n - 1)
            below, above, to_low, to_high = zero, zero, zero, zero
            pieces = {}

            def piece(d, which):
                if abs(d) >= nz:
                    return zero
                if d == 0:
                    return z_out[it, which, rows, :]
                value = z_in[it, (nz - d - 1) % nz if d > 0 else -d - 1, which, rows, :]
                inside = jnp.logical_and(iz + d >= 0, iz + d < nz)
                return jnp.where(inside, value, 0.0)

            own_up = own_dn = zero
            for d in range(-(nz - 1), nz):
                j = iz + d
                inside = jnp.logical_and(j >= 0, j < nz)
                under, over = piece(d - 1, 3), piece(d + 1, 2)
                upt = piece(d, 0) + near * under - over
                dnt = piece(d, 1) + under - near * over
                if d == 0:
                    own_up, own_dn = upt, dnt
                    delta_low, delta_high = under, over
                elif d < 0:
                    below = below + jnp.where(inside, power(n * (-1 - d)) * upt, 0.0)
                else:
                    above = above + jnp.where(inside, power(n * (d - 1)) * dnt, 0.0)
                to_low = to_low + jnp.where(inside, power(n * j + 1) * dnt, 0.0)
                to_high = to_high + jnp.where(inside, power(n * (nz - 1 - j) + 1) * upt, 0.0)
            q = power(n * nz + 1)
            scale = kappa / (1.0 - q * q)
            alpha = kappa * below + (q * to_high - to_low) * scale * power(n * iz)
            beta = kappa * above + (q * to_low - to_high) * scale * power(n * (nz - 1 - iz))
            far = power(n + 1)
            bounds[2, rows, :] = kappa * mu * own_dn + alpha + beta * far
            bounds[3, rows, :] = kappa * mu * own_up + beta + alpha * far
            alpha = alpha + kappa * delta_low * inv
            beta = beta - kappa * delta_high * inv
            bounds[0, rows, :] = kappa * mu * z_out[it, 0, rows, :] + beta
            bounds[1, rows, :] = alpha * power(n)

        strips(body, h)

    def pass_two(it, h):
        last = it == ITERS - 1

        def body(r0):
            rows = pl.ds(r0, ROWS)
            mu, inv = mu_s[rows, :], planes[2, rows, :]
            half = 0.5 * mass[rows, :]
            zero = jnp.zeros((ROWS, nj), jnp.float32)

            def finish(k, above, below, packs):
                p = press[k, rows, :] - half * (above - below)
                if last:
                    press[k, rows, :] = p
                    return packs
                pp[k, pl.ds(PAD + r0, ROWS), :] = p
                return packed(p, k, packs)

            def steps(ks, carry):
                x, h, older, newer, packs = carry
                for k in ks:
                    x = mu * x + vert[k, rows, :]
                    v = x + h
                    h = h * inv
                    vert[k, rows, :] = v
                    geo[k, rows, :] = geo[k, rows, :] + 0.5 * v
                    if not (isinstance(k, int) and k == n - 1):
                        packs = finish(k + 1, older, v, packs)
                    older, newer = newer, v
                return x, h, older, newer, packs

            top = bounds[3, rows, :]
            carry = (bounds[0, rows, :], bounds[1, rows, :], zero, top, (zero, zero))
            carry = steps([n - 1 - e for e in range(unroll)], carry)

            def group(q, carry):
                return steps([n - 1 - q * unroll - e for e in range(unroll)], carry)

            _, _, older, newer, packs = lax.fori_loop(1, n // unroll, group, carry)
            packs = finish(0, older, bounds[2, rows, :], packs)
            if not last:
                for t in range(2):
                    col_out[it + 1, t, rows, :] = packs[t]

        strips(body, h)

    def winds():
        def body(r0):
            rows = pl.ds(r0, ROWS)
            left = col_in[0, 0, rows, :]
            right = col_in[0, 1, rows, :]
            for it in range(1, ITERS):
                left = left + col_in[it, 0, rows, :]
                right = right + col_in[it, 1, rows, :]

            ends = merged(left, right, 1)

            def group(q, carry):
                for e in range(unroll):
                    k = q * unroll + e
                    end = roll(ends[e % 2], nj - 2 - 2 * k)
                    at = pl.ds(PAD + r0, ROWS)
                    p = psum[k, at, :]
                    east[k, rows, :] = up[k, at, :] - 0.25 * (
                        psum[k, pl.ds(PAD + r0 + 1, ROWS), :] - psum[k, pl.ds(PAD + r0 - 1, ROWS), :])
                    low = jnp.where(lane < 1, end, roll(p, 1))
                    high = jnp.where(lane >= nj - 1, end, roll(p, nj - 1))
                    north[k, rows, :] = north[k, rows, :] - 0.25 * (high - low)
                return carry

            lax.fori_loop(0, n // unroll, group, 0)

        strips(body)

    for it in range(ITERS):
        if it > 0:
            recv_rows(it, pp)

        @pl.loop(0, PARTS)
        def _(h, it=it):
            if it > 0:
                for t in range(2):
                    col_copy(it, t, h).wait()
            pass_one(it, h)
            for d in range(1, nz):
                z_copy(it, d, h).start()

        if it == ITERS - 1:
            for t, at in ((0, PAD - 2), (1, PAD + ni)):
                total = row_in[0, t]
                for slot in range(1, ITERS):
                    total = total + row_in[slot, t]
                psum[:, at : at + 2, :] = total
            winds()

        @pl.loop(0, PARTS)
        def _(h, it=it):
            for d in range(1, nz):
                z_copy(it, d, h).wait()
            interface(it, h)
            pass_two(it, h)
            if it < ITERS - 1:
                for t in range(2):
                    col_copy(it + 1, t, h).start()

        if it < ITERS - 1:
            send_rows(it + 1, pp)


def local(sizes, east, north, vert, geo, press, mass):
    n, ni, nj = east.shape
    nz = sizes[2]
    f32 = jnp.float32
    slots = ITERS + 1
    field = pltpu.VMEM((n, ni, nj), f32)
    padded = pltpu.VMEM((n, ni + 2 * PAD, nj), f32)
    plane = pltpu.VMEM((ni, nj), f32)
    return pl.pallas_call(
        functools.partial(kernel, n, ni, nj, sizes),
        out_shape=[pltpu.VMEM((n, ni, nj), f32)] * 5,
        in_specs=[pl.BlockSpec(memory_space=pl.ANY)] * 5 + [pl.BlockSpec(memory_space=pltpu.VMEM)],
        out_specs=[pl.BlockSpec(memory_space=pltpu.VMEM)] * 5,
        scratch_shapes=[
            padded, padded, padded, field, plane, plane,
            pltpu.VMEM((3, ni, nj), f32),
            pltpu.VMEM((4, ni, nj), f32),
            pltpu.VMEM((slots, 2, n, 2, nj), f32),
            pltpu.VMEM((slots, 2, n, 2, nj), f32),
            pltpu.VMEM((slots, 2, ni, nj), f32),
            pltpu.VMEM((slots, 2, ni, nj), f32),
            pltpu.VMEM((ITERS, 4, ni, nj), f32),
            pltpu.VMEM((ITERS, nz - 1, 4, ni, nj), f32),
            pltpu.SemaphoreType.DMA((5,)),
            pltpu.SemaphoreType.DMA((slots, 2)),
            pltpu.SemaphoreType.DMA((slots, 2)),
            pltpu.SemaphoreType.DMA((slots, 2, PARTS)),
            pltpu.SemaphoreType.DMA((slots, 2, PARTS)),
            pltpu.SemaphoreType.DMA((ITERS, nz - 1, PARTS)),
            pltpu.SemaphoreType.DMA((ITERS, nz - 1, PARTS)),
        ],
        compiler_params=pltpu.CompilerParams(
            collective_id=0, has_side_effects=True, vmem_limit_bytes=40 * 1024 * 1024),
    )(east, north, vert, geo, press, mass)


LAG = 5
TILE = 16
WIDE = 32


def paired(n, ni, nj, sizes, east_in, north_in, vert_in, geo_in, press_in, mass_in,
           rhs, star, geo, coef, p0, up, north, edge, faces,
           p1, p2, dvg, head, turned_a, turned_b, turned_c, side, mass, con, packs_p, packs_v,
           row_out, row_in, col_out, col_in, z_out, z_in,
           load_sem, sent, row_recv, col_recv, z_recv):
    nx, ny, _ = sizes
    per = nj // 4
    count = ni // TILE
    press = (p0, p1, p2)
    turned = (turned_a, turned_c, turned_a)
    ix, iy, iz = lax.axis_index("gx"), lax.axis_index("gy"), lax.axis_index("gz")
    xs = (lax.rem(ix + nx - 1, nx), lax.rem(ix + 1, nx))
    ys = (lax.rem(iy + ny - 1, ny), lax.rem(iy + 1, ny))
    flip = (1 - 2 * iz).astype(jnp.float32)
    half = 0.5 * flip
    inner = pl.ds(PAD, ni)

    barrier = pltpu.get_barrier_semaphore()
    for t in range(2):
        pl.semaphore_signal(barrier, inc=1, device_id={"gx": xs[t]})
        pl.semaphore_signal(barrier, inc=1, device_id={"gy": ys[t]})
    pl.semaphore_signal(barrier, inc=1, device_id={"gz": 1 - iz})

    mass_load = pltpu.make_async_copy(mass_in, mass, load_sem.at[5])
    mass_load.start()
    fields = (
        (press_in, p0.at[:, inner, :]), (north_in, north), (east_in, up.at[:, inner, :]),
        (vert_in, head), (geo_in, geo))

    def load(e, m):
        src, dst = fields[e]
        k = iz * (n - 1) + (1 - 2 * iz) * m
        pltpu.make_async_copy(src.at[k], dst.at[m], load_sem.at[e]).start()

    def loaded(e):
        pltpu.make_async_copy(fields[e][0], fields[e][1], load_sem.at[e]).wait()

    @pl.loop(0, n)
    def _(m):
        load(0, m)

    def row_copy(it, t):
        return pltpu.make_async_remote_copy(
            src_ref=row_out.at[it, t], dst_ref=row_in.at[it, 1 - t],
            send_sem=sent.at[0], recv_sem=row_recv.at[it],
            device_id={"gx": xs[t]})

    def arrived(out, inn, e, sem, axis):
        pltpu.make_async_remote_copy(
            src_ref=out, dst_ref=inn, send_sem=sent.at[e], recv_sem=sem,
            device_id={axis: 1 - iz if axis == "gz" else xs[0] if axis == "gx" else ys[0]}).wait_recv()

    def rows_of(s):
        return pl.ds(pl.multiple_of(s * TILE, TILE), TILE)

    def col_copy(it, t, s):
        return pltpu.make_async_remote_copy(
            src_ref=col_out.at[it, t, rows_of(s), :], dst_ref=col_in.at[it, 1 - t, rows_of(s), :],
            send_sem=sent.at[1], recv_sem=col_recv.at[it % 2, s],
            device_id={"gy": ys[t]})

    def z_copy(it, s):
        return pltpu.make_async_remote_copy(
            src_ref=z_out.at[it, :, rows_of(s), :], dst_ref=z_in.at[it, :, rows_of(s), :],
            send_sem=sent.at[2], recv_sem=z_recv.at[it % 2, s],
            device_id={"gz": 1 - iz})

    lane = lax.broadcasted_iota(jnp.int32, (TILE, nj), 1)
    part, couple, quad = lane % 4, lane // 2, lane // 4
    zero = jnp.zeros((TILE, nj), jnp.float32)
    whole = lax.broadcasted_iota(jnp.int32, (ni, nj), 1) % 4

    def placed(mask, value, m, packs):
        b = m // per
        return tuple(jnp.where(mask, value, packs[c]) if c == b else packs[c] for c in range(2))

    def outgoing(it, rows, part, packs):
        a, b = packs
        col_out[it, 0, rows, :] = jnp.where(part >= 2, a, roll(b, -2))
        col_out[it, 1, rows, :] = jnp.where(part < 2, a, roll(b, 2))

    mass_load.wait()
    inverse = 1.0 / (STIFF * mass[...])
    con[0] = 1.25 * inverse
    con[1] = 0.25 * inverse
    base = 2.0 + inverse

    def pivot(m, a):
        load(1, m)
        a = 1.0 / (base - a)
        coef[m] = a
        return a

    last = lax.fori_loop(0, n, pivot, jnp.zeros((ni, nj), jnp.float32))
    con[2] = last / (1.0 - last * last)

    wide = lax.broadcasted_iota(jnp.int32, (WIDE, nj), 1)
    blank = jnp.zeros((WIDE, nj), jnp.float32)
    share = n * WIDE // ni

    loaded(0)

    @pl.loop(0, ni // WIDE)
    def _(b):
        r0 = pl.multiple_of(b * WIDE, WIDE)
        rows = pl.ds(r0, WIDE)
        packs = (blank, blank)
        for m in range(n):
            value = roll(p0[m, pl.ds(PAD + r0, WIDE), :], 4 * (m % per) + 2)
            turned_a[m, rows, :] = value
            packs = placed(wide // 4 == m % per, value, m, packs)
            if m < share:
                load(2, b * share + m)
        packs_p[0, rows, :], packs_p[1, rows, :] = packs

    loaded(1)

    @pl.loop(0, ni // WIDE)
    def _(b):
        r0 = pl.multiple_of(b * WIDE, WIDE)
        rows = pl.ds(r0, WIDE)
        packs = (blank, blank)
        for m in range(n):
            q = 4 * (m % per)
            value = roll(4.0 * north[m, rows, :], q + 1)
            turned_b[m, rows, :] = turned_a[m, rows, :] + value
            packs = placed(wide // 2 == q // 2, value, m, packs)
            if m < share:
                load(3, b * share + m)
                load(4, b * share + m)
        packs_v[0, rows, :], packs_v[1, rows, :] = packs

    edges = []
    for c in range(2):
        v = packs_v[c]
        back = roll(v, 2)
        edges.append(packs_p[c] + jnp.where(whole == 0, v, jnp.where(whole == 3, -back, 0.0)))
        packs_v[c] = jnp.where(whole == 1, v, jnp.where(whole == 2, -back, 0.0))
    outgoing(0, slice(None), whole, edges)

    pl.semaphore_wait(barrier, 5)

    @pl.loop(0, count)
    def _(t):
        s = lax.rem(t + 1, count)
        for t in range(2):
            col_copy(0, t, s).start()

    loaded(2)
    up[:, :PAD, :] = jnp.zeros((n, PAD, nj), jnp.float32)
    up[:, PAD + ni :, :] = jnp.zeros((n, PAD, nj), jnp.float32)
    row_out[0, 0] = p0[:, PAD : PAD + 2, :] - 4.0 * up[:, PAD - 1 : PAD + 1, :]
    row_out[0, 1] = p0[:, PAD + ni - 2 : PAD + ni, :] + 4.0 * up[:, PAD + ni - 1 : PAD + ni + 1, :]
    for t in range(2):
        row_copy(0, t).start()

    @pl.loop(0, ni // WIDE)
    def _(b):
        rows = pl.ds(pl.multiple_of(b * WIDE, WIDE), WIDE)
        for m in range(n):
            turned_a[m, rows, :] = turned_a[m, rows, :] - roll(4.0 * north[m, rows, :], 4 * (m % per) + 3)

    loaded(3)
    loaded(4)

    def lateral(it, s):
        rows = rows_of(s)
        left, right = col_in[it, 0, rows, :], col_in[it, 1, rows, :]
        ends = (jnp.where(part < 2, left, right), jnp.where(part < 2, roll(left, -2), roll(right, 2)))
        if it == 0:
            ends = [ends[c] + packs_v[c, rows, :] for c in range(2)]

        def level(m):
            q, end = m % per, ends[m // per]
            lower = upper = turned[it][m, rows, :]
            if it == 0:
                lower = turned_b[m, rows, :]
            low = roll(jnp.where(couple == 2 * q, end, lower), -4 * q)
            high = roll(jnp.where(couple == 2 * q + 1, end, upper), -4 * q - 4)
            side[m] = low + high

        return level

    def forward(it, s):
        rows = rows_of(s)
        r0 = PAD + pl.multiple_of(s * TILE, TILE)
        at = pl.ds(r0, TILE)
        weak = 0.05 * mass[rows, :]
        four = 4.0 * weak
        state = {"older": zero, "newer": None, "g": None}

        def close(m, above):
            own = head[m, rows, :]
            if it == 0:
                own = flip * own + half * geo[m, rows, :]
            g = own - (above - state["older"])
            if m > 0:
                g = g + coef[m - 1, rows, :] * state["g"]
            rhs[m, rows, :] = g
            state["g"] = g

        def level(m):
            ref = press[it]
            p = ref[m, at, :]
            total = (ref[m, pl.ds(r0 + 2, TILE), :] + ref[m, pl.ds(r0 - 2, TILE), :]) + side[m]
            d = four * p
            if it == 0:
                total = total - 4.0 * (up[m, pl.ds(r0 + 1, TILE), :] - up[m, pl.ds(r0 - 1, TILE), :])
            else:
                d = dvg[m, rows, :] + d
            d = d - weak * total
            if it < ITERS - 1:
                dvg[m, rows, :] = d
            else:
                p0[m, at, :] = (p0[m, at, :] + p1[m, at, :]) + p
            ps = p - d
            star[m, rows, :] = ps
            if m > 0:
                close(m - 1, ps)
                state["older"] = state["newer"]
            state["newer"] = ps

        def finish():
            close(n - 1, zero)
            z_out[it, 0, rows, :] = state["g"]
            z_out[it, 1, rows, :] = state["newer"]
            z_copy(it, s).start()

        return level, finish

    def col_wait(it, s):
        arrived(col_out.at[it, :, rows_of(s), :], col_in.at[it, :, rows_of(s), :], 1, col_recv.at[it % 2, s], "gy")

    def row_wait(it):
        arrived(row_out.at[it], row_in.at[it], 0, row_recv.at[it], "gx")
        press[it][:, PAD - 2 : PAD, :] = row_in[it, 0]
        press[it][:, PAD + ni : PAD + ni + 2, :] = row_in[it, 1]

    def meet(a, w, out, inn):
        mine, other = out[0] - inn[1], inn[0] - out[1]
        z = w * (mine - a * other)
        return z, a * (z - other)

    def backward(it, s):
        rows = rows_of(s)
        at = pl.ds(PAD + pl.multiple_of(s * TILE, TILE), TILE)
        near, far = con[0, rows, :], con[1, rows, :]
        z_copy(it, s).wait_recv()
        state = {"packs": (zero, zero)}
        state["z"], state["above"] = meet(
            coef[n - 1, rows, :], con[2, rows, :],
            [z_out[it, c, rows, :] for c in range(2)], [z_in[it, c, rows, :] for c in range(2)])

        def level(m):
            z = state["z"]
            g = geo[m, rows, :]
            if it == 0:
                g = half * g
            head[m, rows, :] = near * z + g
            geo[m, rows, :] = far * z + g
            below = coef[m - 1, rows, :] * (rhs[m - 1, rows, :] + z) if m > 0 else zero
            p = star[m, rows, :] - (0.5 / STIFF) * (state["above"] - below)
            press[it + 1][m, at, :] = p
            value = roll(p, 4 * (m % per) + 2)
            turned[it + 1][m, rows, :] = value
            state["packs"] = placed(quad == m % per, value, m, state["packs"])
            state["above"], state["z"] = z, below

        def finish():
            outgoing(it + 1, rows, part, state["packs"])
            for t in range(2):
                col_copy(it + 1, t, s).start()

        return level, finish

    for it in range(ITERS):
        final = it == ITERS - 1
        front = (count - 2, count - 2, count - 2)[it]
        lag = count if final else LAG

        def order(t, front=front):
            return jnp.where(t < front, t + 1, jnp.where(t == front, count - 1, jnp.where(t == front + 1, 0, t - 1)))

        def ahead_of(t, it=it, front=front, order=order):
            @pl.when(t == front)
            def _():
                row_wait(it)

            after = order(lax.rem(t + 1, count))

            @pl.when(t < count - 1)
            def _():
                col_wait(it, after)

            return forward(it, order(t)) + (lateral(it, after),)

        def behind(u, it=it, order=order):
            return backward(it, order(u))

        def send_rows(u, it=it, front=front):
            @pl.when(u == front)
            def _():
                row_out[it + 1, 1] = press[it + 1][:, PAD + ni - 2 : PAD + ni, :]
                row_copy(it + 1, 1).start()

            @pl.when(u == front + 1)
            def _():
                row_out[it + 1, 0] = press[it + 1][:, PAD : PAD + 2, :]
                row_copy(it + 1, 0).start()

        col_wait(it, order(0))
        first = lateral(it, order(0))
        for m in range(n):
            first(m)

        @pl.loop(0, lag)
        def _(t):
            one, finish, ahead = ahead_of(t)
            for m in range(n):
                one(m)
                ahead(m)
            finish()

        if not final:
            @pl.loop(lag, count)
            def _(t):
                one, finish, ahead = ahead_of(t)
                for m in range(n):
                    one(m)
                    ahead(m)
                finish()
                two, deliver = behind(t - lag)
                for m in range(n):
                    two(n - 1 - m)
                deliver()
                send_rows(t - lag)

            @pl.loop(count - lag, count)
            def _(u):
                two, deliver = behind(u)
                for m in range(n):
                    two(n - 1 - m)
                deliver()
                send_rows(u)

    for t, at in ((0, PAD - 2), (1, PAD + ni)):
        p0[:, at : at + 2, :] = (row_in[0, t] + row_in[1, t]) + row_in[2, t]
    left = (col_in[0, 0] + col_in[1, 0]) + col_in[2, 0]
    right = (col_in[0, 1] + col_in[1, 1]) + col_in[2, 1]
    edge[0] = jnp.where(whole == 1, roll(right, -1), roll(left, 1))
    edge[1] = jnp.where(whole == 1, roll(right, 1), roll(left, -1))

    @pl.loop(0, count)
    def _(s):
        z_copy(ITERS - 1, s).wait_recv()

    faces[0], faces[1] = meet(
        coef[n - 1], con[2], [z_out[ITERS - 1, c] for c in range(2)], [z_in[ITERS - 1, c] for c in range(2)])

    for e, out, inn, axis in ((0, row_out, row_in, "gx"), (1, col_out, col_in, "gy"), (2, z_out, z_in, "gz")):
        pltpu.make_async_remote_copy(
            src_ref=out, dst_ref=inn, send_sem=sent.at[e], recv_sem=load_sem.at[e],
            device_id={axis: 1 - iz if axis == "gz" else xs[0] if axis == "gx" else ys[0]}).wait_send()


def finale(n, ni, nj, rhs, star, geo, coef, psum, up, north, edge, faces, mass,
           east_out, north_out, vert_out, geo_out, press_out,
           east_s, north_s, vert_s, geo_s, press_s, sem):
    per = nj // 4
    count = ni // WIDE
    iz = lax.axis_index("gz")
    flip = (1 - 2 * iz).astype(jnp.float32)
    lane = lax.broadcasted_iota(jnp.int32, (WIDE, nj), 1)

    def store(e, src, dst, rows):
        return pltpu.make_async_copy(src.at[:, rows, :], dst.at[:, rows, :], sem.at[e])

    outs = ((east_s, east_out), (north_s, north_out), (vert_s, vert_out), (geo_s, geo_out), (press_s, press_out))

    def level_of(m):
        return iz * (n - 1) + (1 - 2 * iz) * m

    @pl.loop(0, count)
    def _(s):
        rows = pl.ds(pl.multiple_of(s * WIDE, WIDE), WIDE)
        v_of = flip / (STIFF * mass[rows, :])
        half = 0.5 * v_of
        twice = 2.0 * flip
        z, above = faces[0, rows, :], faces[1, rows, :]
        for m in range(n - 1, -1, -1):
            k = level_of(m)
            vert_s[k, rows, :] = v_of * z
            geo_s[k, rows, :] = twice * geo[m, rows, :] + half * z
            below = coef[m - 1, rows, :] * (rhs[m - 1, rows, :] + z) if m > 0 else jnp.zeros_like(z)
            press_s[k, rows, :] = star[m, rows, :] - (0.5 / STIFF) * (above - below)
            above, z = z, below
        for e in (2, 3, 4):
            store(e, *outs[e], rows).start()

    @pl.loop(0, count)
    def _(s):
        rows = pl.ds(pl.multiple_of(s * WIDE, WIDE), WIDE)
        r0 = PAD + pl.multiple_of(s * WIDE, WIDE)
        ends = (edge[0, rows, :], edge[1, rows, :])
        for m in range(n):
            k = level_of(m)
            p = psum[m, pl.ds(r0, WIDE), :]
            end = roll(ends[m // per], nj - 2 - 4 * (m % per))
            low = jnp.where(lane < 1, end, roll(p, 1))
            high = jnp.where(lane >= nj - 1, end, roll(p, nj - 1))
            north_s[k, rows, :] = north[m, rows, :] - 0.25 * (high - low)
            east_s[k, rows, :] = up[m, pl.ds(r0, WIDE), :] - 0.25 * (
                psum[m, pl.ds(r0 + 1, WIDE), :] - psum[m, pl.ds(r0 - 1, WIDE), :])
        for e in (0, 1):
            store(e, *outs[e], rows).start()

    for e in range(5):
        pltpu.make_async_copy(outs[e][0], outs[e][1], sem.at[e]).wait()


def pair(sizes, east, north, vert, geo, press, mass):
    n, ni, nj = east.shape
    f32 = jnp.float32
    count = ni // TILE
    shape = (n, ni, nj)
    padded = (n, ni + 2 * PAD, nj)
    kept = [shape, shape, shape, shape, padded, padded, shape, (2, ni, nj), (2, ni, nj)]
    vmem = pl.BlockSpec(memory_space=pltpu.VMEM)
    state = pl.pallas_call(
        functools.partial(paired, n, ni, nj, sizes),
        out_shape=[pltpu.VMEM(s, f32) for s in kept],
        in_specs=[pl.BlockSpec(memory_space=pltpu.HBM)] * 6,
        out_specs=[vmem] * len(kept),
        scratch_shapes=[
            pltpu.VMEM(padded, f32), pltpu.VMEM(padded, f32), pltpu.VMEM(shape, f32), pltpu.VMEM(shape, f32),
            pltpu.VMEM(shape, f32), pltpu.VMEM(shape, f32), pltpu.VMEM(shape, f32),
            pltpu.VMEM((n, TILE, nj), f32),
            pltpu.VMEM((ni, nj), f32),
            pltpu.VMEM((3, ni, nj), f32),
            pltpu.VMEM((2, ni, nj), f32),
            pltpu.VMEM((2, ni, nj), f32),
            pltpu.VMEM((ITERS, 2, n, 2, nj), f32),
            pltpu.VMEM((ITERS, 2, n, 2, nj), f32),
            pltpu.VMEM((ITERS, 2, ni, nj), f32),
            pltpu.VMEM((ITERS, 2, ni, nj), f32),
            pltpu.VMEM((ITERS, 2, ni, nj), f32),
            pltpu.VMEM((ITERS, 2, ni, nj), f32),
            pltpu.SemaphoreType.DMA((6,)),
            pltpu.SemaphoreType.DMA((3,)),
            pltpu.SemaphoreType.DMA((ITERS,)),
            pltpu.SemaphoreType.DMA((2, count)),
            pltpu.SemaphoreType.DMA((2, count)),
        ],
        compiler_params=pltpu.CompilerParams(
            collective_id=0, has_side_effects=True, vmem_limit_bytes=41 * 1024 * 1024),
    )(east, north, vert, geo, press, mass)
    return pl.pallas_call(
        functools.partial(finale, n, ni, nj),
        out_shape=[jax.ShapeDtypeStruct(shape, f32)] * 5,
        in_specs=[vmem] * (len(kept) + 1),
        out_specs=[pl.BlockSpec(memory_space=pl.ANY)] * 5,
        scratch_shapes=[pltpu.VMEM(shape, f32)] * 5 + [pltpu.SemaphoreType.DMA((5,))],
        compiler_params=pltpu.CompilerParams(vmem_limit_bytes=18 * 1024 * 1024),
    )(*state, mass)


def solution(mesh):
    sizes = (mesh.shape["gx"], mesh.shape["gy"], mesh.shape["gz"])
    cube = P("gz", "gx", "gy")

    def body(east, *rest):
        n, ni, nj = east.shape
        fits = sizes[2] == 2 and n <= nj // 2 and ni % TILE == 0 and ni // TILE > LAG and ni % WIDE == 0 and n * WIDE % ni == 0 and ITERS == 3
        return (pair if fits else local)(sizes, east, *rest)

    return jax.shard_map(
        body, mesh=mesh,
        in_specs=(cube,) * 5 + (P("gx", "gy"),), out_specs=(cube,) * 5, check_vma=False)
```
